256 devices in a mesh: dp: 4 (over y), expert: 16 (over z, core), pipe: 4 (over x).
Axes of the slice: x: 4, y: 4, z: 8, core: 2. Of those that a mesh axis runs over, the one named last changes fastest.
Arguments:
- inputs: bfloat16 [2048, 4096], P('expert'), may hold values from -6 to 6
- cotangents: bfloat16 [2048, 4096], P('expert'), may hold values from -6 to 6
- routes: int32 [2048, 2], P('expert'), may hold values from 0 to 15, all different within a row; in each aligned block of 128 rows (0 to 127, 128 to 255, ...) at most 32 rows name the same one
- gates: float32 [2048, 2], P('expert'), may hold values from 0.1 to 1
- w_gate: bfloat16 [16, 4096, 7168], P('expert', None, ('dp', 'pipe')), may hold values from -0.09375 to 0.09375
- w_up: bfloat16 [16, 4096, 7168], P('expert', None, ('dp', 'pipe')), may hold values from -0.09375 to 0.09375
- w_down: bfloat16 [16, 7168, 4096], P('expert', ('dp', 'pipe')), may hold values from -0.09375 to 0.09375
- proj_in: bfloat16 [4096, 32], replicated, may hold values from -0.09375 to 0.09375
- proj_out: bfloat16 [4096, 64], replicated, may hold values from -0.09375 to 0.09375
- proj_hid_a: bfloat16 [7168, 32], P(('dp', 'pipe')), may hold values from -0.0625 to 0.0625
- proj_hid_b: bfloat16 [7168, 64], P(('dp', 'pipe')), may hold values from -0.0625 to 0.0625
- queries: bfloat16 [256, 6144], P(('dp', 'pipe')), may hold values from -0.078125 to 0.078125
Outputs:
- token_scores: float32 [2048, 256], P('expert', ('dp', 'pipe'))
- query_totals: float32 [256], P(('dp', 'pipe'))
The draws below stay inside these ranges and needn't reach their ends.
Inputs may be any that keep to these rules, and one draw needn't show every extreme that they name: `routes`: each row names two different experts. Among the 128 tokens of one index of expert (aligned blocks), no expert is named more than 32 times, and in some blocks one expert is named exactly 32 times.
All inputs are finite; a program needn't handle non-finite values.
Results may differ from the reference program's by a relative error of at most 0.0041.
Values may be sent and summed in bfloat16 or wider, within the bound.
A program may use at most 128 MiB of HBM per device.

```python
import math
import jax
import jax.numpy as jnp
import numpy as np
from jax import lax

D = 4096
FF = 7168
KA = 32
KB = 64
NQ = 256
TOK_DEV = 128
EXPERTS = 16
TOKENS = 2048
CAP = 32
SKETCH = 6144
N_EXPERT = 16


def block_levels(stream_key, extent, pieces, low, top_value):
    def one(dim, shards_of):
        steps = jax.random.uniform(jax.random.fold_in(jax.random.fold_in(stream_key, 6), dim), (shards_of,), jnp.float32, low / len(pieces), top_value / len(pieces))
        return jnp.repeat(jnp.exp(steps), extent[dim] // shards_of).reshape((-1,) + (1,) * (len(extent) - dim - 1))

    gain = one(*pieces[0])
    for cut in pieces[1:]:
        gain = gain * one(*cut)
    return gain


def shared_out(stream_key, own, number, rows, count, top, bound, skew):
    order = jax.random.permutation(stream_key, count)
    crowded, common = portions_of(count, rows * top, bound, skew, True), portions_of(count, rows * top, bound, skew, False)
    places = jnp.arange(count)

    def named(sizes, rotation):
        used = int((sizes > 0).sum())
        fixed = max(1, used // 4)
        passed = fixed + (places - fixed + rotation * (used - fixed)) % max(1, count - fixed)
        return jnp.zeros((count,), jnp.int32).at[order[jnp.where(places < fixed, places, passed)]].set(jnp.asarray(sizes, jnp.int32))

    sizes = jnp.where(number % 4 == 0, named(crowded, number // 4), named(common, number - number // 4 - 1))
    mixed = jax.random.permutation(jax.random.fold_in(own, 3), count)
    source_of, taker = mixed[0:count // 2 * 2:2], mixed[1:count // 2 * 2:2]
    room = jnp.minimum(sizes[source_of] - 1, bound - sizes[taker]) // 2
    room = jnp.where((source_of == order[0]) | (taker == order[0]) | (sizes[taker] == 0), 0, jnp.maximum(room, 0))
    passed = jax.random.randint(jax.random.fold_in(own, 4), (count // 2,), 0, 1 << 20) % (room + 1)
    sizes = sizes.at[source_of].add(-passed).at[taker].add(passed)
    items = jnp.searchsorted(jnp.cumsum(sizes), jnp.arange(rows * top), side="right").astype(jnp.int32)
    table = items.reshape(top, rows).T
    table = table[jax.random.permutation(jax.random.fold_in(own, 1), rows)]
    rotation = jax.random.randint(jax.random.fold_in(own, 2), (rows, 1), 0, top)
    return jnp.take_along_axis(table, (jnp.arange(top)[None, :] + rotation) % top, axis=1)


def portions_of(count, total, bound, slope, full):
    loads = [(1 << 20) // math.isqrt(rank ** slope) + 1 for rank in range(1, count + 1)]
    largest = bound if full else min(bound, max(-(-total // count), total * loads[0] // sum(loads)))
    least = 1 if total - largest >= count - 1 else 0
    given, surplus = [largest] + [least] * (count - 1), total - largest - least * (count - 1)
    while surplus > 0:
        candidates = [i for i in range(1, count) if given[i] < largest] or [i for i in range(1, count) if given[i] < bound]
        pool, left = sum([loads[i] for i in candidates]), surplus
        for i in candidates:
            more = min(bound - given[i], max(1, left * loads[i] // pool), surplus)
            given[i] = given[i] + more
            surplus = surplus - more
    return np.array(given)


def scatter_about(rng, dims, deviation, most, shards=(), kind=jnp.bfloat16):
    drawn = deviation * jax.random.normal(rng, dims, jnp.float32)
    if shards:
        drawn = drawn * block_levels(rng, dims, shards, -0.22, 0.18)
    return jnp.clip(drawn, -most, most).astype(kind)


def setup_inputs(seed: int = 0) -> dict:
    splits = jax.random.split(jax.random.key(seed), 13)
    inputs = scatter_about(splits[0], (TOKENS, D), 1.0, 6.0, ((0, 16),))
    cotangents = scatter_about(splits[1], (TOKENS, D), 1.0, 6.0, ((0, 16),))
    routes_keys = jax.random.split(jax.random.fold_in(splits[2], 1), TOKENS // TOK_DEV)
    routes_turns = jax.random.permutation(jax.random.fold_in(splits[2], 3), TOKENS // TOK_DEV)
    routes = jax.vmap(lambda own, number: shared_out(jax.random.fold_in(splits[2], 2), own, number, TOK_DEV, EXPERTS, 2, CAP, 2))(routes_keys, routes_turns).reshape((TOKENS, 2))
    gates = jnp.clip(jnp.exp(math.log(1.0) - 2.3025851 * jax.random.uniform(splits[3], (TOKENS, 2), jnp.float32) ** block_levels(splits[3], (TOKENS, 2), ((0, 16),), -0.2, 0.2)), 0.1, 1.0)
    w_gate = scatter_about(splits[4], (EXPERTS, D, FF), D ** -0.5, 0.09375, ((0, 16), (2, 16)))
    w_up = scatter_about(splits[5], (EXPERTS, D, FF), D ** -0.5, 0.09375, ((0, 16), (2, 16)))
    w_down = scatter_about(splits[6], (EXPERTS, FF, D), D ** -0.5, 0.09375, ((0, 16), (1, 16)))
    proj_in = scatter_about(splits[7], (D, KA), D ** -0.5, 0.09375)
    proj_out = scatter_about(splits[8], (D, KB), D ** -0.5, 0.09375)
    proj_hid_a = scatter_about(splits[9], (FF, KA), FF ** -0.5, 0.0625, ((0, 16),))
    proj_hid_b = scatter_about(splits[10], (FF, KB), FF ** -0.5, 0.0625, ((0, 16),))
    queries = scatter_about(splits[11], (NQ, SKETCH), SKETCH ** -0.5, 0.078125, ((0, 16),))
    return dict(inputs=inputs, cotangents=cotangents, routes=routes, gates=gates, w_gate=w_gate, w_up=w_up, w_down=w_down, proj_in=proj_in, proj_out=proj_out, proj_hid_a=proj_hid_a, proj_hid_b=proj_hid_b, queries=queries)


def slot_matrix(route_rows, gate_rows, experts, capacity):
    count = route_rows.shape[0]
    flat = route_rows.reshape(-1)
    labels = jnp.arange(experts, dtype=jnp.int32)
    onehot = (flat[:, None] == labels[None, :]).astype(jnp.int32)
    earlier = jnp.cumsum(onehot, axis=0) - onehot
    position = lax.optimization_barrier(jnp.sum(onehot * (labels[None, :] * capacity + earlier), axis=1))
    slot_ids = jnp.arange(experts * capacity, dtype=jnp.int32)
    table = (position[None, :] == slot_ids[:, None]).astype(jnp.float32).reshape(experts * capacity, count, 2)
    picks = lax.optimization_barrier(jnp.sum(table, axis=2))
    weighted = lax.optimization_barrier(jnp.sum(table * gate_rows[None, :, :], axis=2))
    return (picks, weighted)

def expert_scores(rows_in, rows_back, gate_proj, up_proj, down_proj, input_proj, output_proj, hidden_proj, grad_proj, query_rows):
    gate_pre = jnp.dot(rows_in, gate_proj, preferred_element_type=jnp.float32)
    up_pre = jnp.dot(rows_in, up_proj, preferred_element_type=jnp.float32)
    sigma = jax.nn.sigmoid(gate_pre)
    hidden = (gate_pre * sigma * up_pre).astype(jnp.bfloat16)
    a_input = jnp.dot(rows_in, input_proj, preferred_element_type=jnp.float32)
    a_hidden = jnp.dot(hidden, hidden_proj, preferred_element_type=jnp.float32)
    back = lax.dot_general(rows_back, down_proj, (((1,), (1,)), ((), ())), preferred_element_type=jnp.float32)
    d_up = (back * gate_pre * sigma).astype(jnp.bfloat16)
    d_gate = (back * up_pre * sigma * (1.0 + gate_pre * (1.0 - sigma))).astype(jnp.bfloat16)
    b_output = jnp.dot(rows_back, output_proj, preferred_element_type=jnp.float32)
    b_up = jnp.dot(d_up, grad_proj, preferred_element_type=jnp.float32)
    b_gate = jnp.dot(d_gate, grad_proj, preferred_element_type=jnp.float32)
    height = rows_back.shape[0]
    sketch = jnp.concatenate([(a_hidden[:, :, None] * b_output[:, None, :]).reshape(height, -1), (a_input[:, :, None] * b_up[:, None, :]).reshape(height, -1), (a_input[:, :, None] * b_gate[:, None, :]).reshape(height, -1)], axis=1).astype(jnp.bfloat16)
    return lax.dot_general(sketch, query_rows, (((1,), (1,)), ((), ())), preferred_element_type=jnp.float32)

def reference(inputs, cotangents, routes, gates, w_gate, w_up, w_down, proj_in, proj_out, proj_hid_a, proj_hid_b, queries):
    sources = N_EXPERT
    rows_in = inputs.reshape(sources, TOK_DEV, D)
    rows_back = cotangents.reshape(sources, TOK_DEV, D)
    picks, weighted = jax.vmap(lambda r, g: slot_matrix(r, g, EXPERTS, CAP))(routes.reshape(sources, TOK_DEV, 2), gates.reshape(sources, TOK_DEV, 2))

    def dispatch(index):
        pick = picks[index].astype(jnp.bfloat16)
        first = jnp.dot(pick, rows_in[index], preferred_element_type=jnp.float32).astype(jnp.bfloat16)
        second = jnp.dot(pick, rows_back[index], preferred_element_type=jnp.float32).astype(jnp.bfloat16)
        return (first, second)
    slots_in, slots_back = lax.map(dispatch, jnp.arange(sources, dtype=jnp.int32))
    slots_in = slots_in.reshape(sources, EXPERTS, CAP, D).transpose(1, 0, 2, 3).reshape(EXPERTS, sources * CAP, D)
    slots_back = slots_back.reshape(sources, EXPERTS, CAP, D).transpose(1, 0, 2, 3).reshape(EXPERTS, sources * CAP, D)

    def per_expert(expert):
        return expert_scores(slots_in[expert], slots_back[expert], w_gate[expert], w_up[expert], w_down[expert], proj_in, proj_out, proj_hid_a, proj_hid_b, queries)
    scores = lax.map(per_expert, jnp.arange(EXPERTS, dtype=jnp.int32))
    scores = scores.reshape(EXPERTS, sources, CAP, NQ).transpose(1, 0, 2, 3).reshape(sources, EXPERTS * CAP, NQ)

    def combine(index):
        return lax.dot_general(weighted[index], scores[index], (((0,), (0,)), ((), ())), precision=lax.Precision.HIGHEST, preferred_element_type=jnp.float32)
    token_scores = lax.map(combine, jnp.arange(sources, dtype=jnp.int32)).reshape(TOKENS, NQ)
    query_totals = lax.optimization_barrier(jnp.sum(token_scores, axis=0)) * (1.0 / math.sqrt(TOKENS))
    return (token_scores, query_totals)
```

```python
import math

import jax
import jax.numpy as jnp
from jax import lax
from jax.experimental import pallas as pl
from jax.experimental.pallas import tpu as pltpu
from jax.sharding import PartitionSpec as P

MESH = pl.DeviceIdType.MESH
F32, BF16, I32 = jnp.float32, jnp.bfloat16, jnp.int32

NZ = 8
ORDER = (1, 7, 2, 6, 3, 5, 0, 4)
LOCAL = ORDER.index(0)
SLOTS = 32
COLS = 256
SHARES = 16
GROUPS = ((0, 4), (4, 4), (8, 4), (14, 2))
PLANE = sorted(
    ((dy, dx) for dy in range(4) for dx in range(4) if dy or dx),
    key=lambda o: min(o[0], 4 - o[0]) + min(o[1], 4 - o[1]),
)


def nn(a, b):
    return lax.dot_general(a, b, (((1,), (0,)), ((), ())), preferred_element_type=F32)


def nt(a, b):
    return lax.dot_general(a, b, (((1,), (1,)), ((), ())), preferred_element_type=F32)


def iota(shape, dim):
    return lax.broadcasted_iota(I32, shape, dim)


def split(v):
    high = v.astype(BF16)
    return high, (v - high.astype(F32)).astype(BF16)


def kernel(
    x_hbm, g_hbm, routes_hbm, gates_hbm, wg_hbm, wu_hbm, wd_hbm, pin_hbm, pout_hbm, pa_hbm, pb_hbm, q_hbm,
    tok_ref, tot_ref,
    xs, gs, routes, gates, wg, wu, wd, pa, pb, qs,
    full, out_rows, out_pair, acc0, acc1, acc2, keep_in, keep_out,
    pat, pbt1, pbt2, wq0, wq12, wm_hi, wm_lo, wrow, wrecv,
    part, gathered, own, factors, score_send, score_recv, tot_send, tot_recv,
    load_sem, z_send, z_recv, pair_send, pair_recv, w_send, w_recv,
    g_send, g_recv, rs_send, rs_recv, ag_send, ag_recv, sc_send, sc_recv, t_send, t_recv,
):
    y, e, x = lax.axis_index("dp"), lax.axis_index("expert"), lax.axis_index("pipe")
    z, c = lax.div(e, 2), lax.rem(e, 2)
    other = 1 - c
    me = y * 4 + x

    def device(yy, ee, xx):
        return {"dp": yy, "expert": ee, "pipe": xx}

    def column(pos, core):
        return device(y, lax.rem(z + ORDER[pos], NZ) * 2 + core, x)

    def back_column(pos, core):
        return device(y, lax.rem(z + NZ - ORDER[pos], NZ) * 2 + core, x)

    def plane(dy, dx):
        return device(lax.rem(y + dy, 4), e, lax.rem(x + dx, 4))

    def plane_index(dy, dx):
        return lax.rem(y + dy, 4) * 4 + lax.rem(x + dx, 4)

    sent = []

    def remote(src, dst, ss, rs, dev):
        copy = pltpu.make_async_remote_copy(
            src_ref=src, dst_ref=dst, send_sem=ss, recv_sem=rs, device_id=dev, device_id_type=MESH
        )
        copy.start()
        sent.append(copy)

    def arrived(dst, rs):
        pltpu.make_async_remote_copy(
            src_ref=dst, dst_ref=dst, send_sem=rs, recv_sem=rs, device_id=device(y, e, x), device_id_type=MESH
        ).wait_recv()

    barrier = pltpu.get_barrier_semaphore()
    for dy, dx in PLANE:
        pl.semaphore_signal(barrier, inc=1, device_id=plane(dy, dx), device_id_type=MESH)
    for pos in range(NZ):
        if pos == LOCAL:
            pl.semaphore_signal(barrier, inc=1, device_id=column(pos, other), device_id_type=MESH)
        else:
            for core in range(2):
                pl.semaphore_signal(barrier, inc=1, device_id=column(pos, core), device_id_type=MESH)

    loads = {}
    for i, (name, src, dst) in enumerate(
        (
            ("routes", routes_hbm, routes),
            ("gates", gates_hbm, gates),
            ("x", x_hbm, xs),
            ("g", g_hbm, gs),
            ("q", q_hbm, qs),
            ("pa", pa_hbm, pa),
            ("pb", pb_hbm, pb),
            ("pin", pin_hbm, wg.at[448:480]),
            ("pout", pout_hbm, wd.at[448:512]),
            ("wg", wg_hbm, wg.at[0:448]),
            ("wu", wu_hbm, wu),
            ("wd", wd_hbm, wd.at[0:448]),
        )
    ):
        loads[name] = pltpu.make_async_copy(src, dst, load_sem.at[i])
        loads[name].start()

    loads["routes"].wait()
    loads["gates"].wait()
    first, second = routes[0:1, :], routes[1:2, :]
    expert_rows = iota((16, 128), 0)
    named = ((expert_rows == first) | (expert_rows == second)).astype(F32)
    before = (iota((128, 128), 0) < iota((128, 128), 1)).astype(F32)
    earlier = nn(named.astype(BF16), before.astype(BF16))

    def places(route):
        slot = jnp.sum(jnp.where(expert_rows == route, earlier, 0.0), axis=0, keepdims=True).astype(I32)
        offset = ((route >> 1) - z) & (NZ - 1)
        pos = jnp.zeros_like(offset)
        for i, o in enumerate(ORDER):
            pos = jnp.where(offset == o, i, pos)
        block = pos * 2 + (route & 1)
        lane = block * 128 + ((pos & 1) * 2 + c) * 32 + slot
        return block * SLOTS + slot, lane

    place0, lane0 = places(first)
    place1, lane1 = places(second)

    def picks_of(start, count):
        rows = iota((count, 128), 0) + start
        return ((rows == place0) | (rows == place1)).astype(F32).astype(BF16)

    picks = picks_of(0, 512)
    shares = (y * 4 + x, x * 4 + y)
    for a, (name, source) in enumerate((("x", xs), ("g", gs))):
        loads[name].wait()
        columns = pl.ds(pl.multiple_of(shares[a] * COLS, COLS), COLS)
        rows = nn(picks, source[:, columns]).astype(BF16)
        out_rows[a] = rows.reshape(16, SLOTS, COLS)
    pair_picks = picks_of((2 * LOCAL + other) * SLOTS, SLOTS)
    for a, source in enumerate((xs, gs)):
        for p in range(SHARES):
            out_pair[a, p] = nn(pair_picks, source[:, p * COLS : (p + 1) * COLS]).astype(BF16)

    pl.semaphore_wait(barrier, 30)

    for pos in range(NZ):
        if pos == LOCAL:
            continue
        for a in range(2):
            for core in range(2):
                remote(
                    out_rows.at[a, 2 * pos + core],
                    full.at[a, shares[a], 2 * pos + c],
                    z_send.at[a, 2 * pos + core],
                    z_recv.at[a, 2 * pos + c],
                    column(pos, core),
                )
    for a in range(2):
        remote(
            out_pair.at[a],
            full.at[a, :, 2 * LOCAL + c],
            pair_send.at[a],
            pair_recv.at[a],
            device(y, z * 2 + other, x),
        )

    own_picks = picks_of((2 * LOCAL + c) * SLOTS, SLOTS)
    for a, source in enumerate((xs, gs)):
        for p in range(SHARES):
            full[a, p, 2 * LOCAL + c] = nn(own_picks, source[:, p * COLS : (p + 1) * COLS]).astype(BF16)

    lanes = iota((2048, 128), 0)
    weights = jnp.where(lanes == lane0, gates[0:1, :], 0.0) + jnp.where(lanes == lane1, gates[1:2, :], 0.0)
    high, low = split(weights)
    wm_hi[...] = high
    wm_lo[...] = low
    ones = jnp.ones((8, 128), BF16)
    sums = nt(ones, high) + nt(ones, low)
    for k in range(16):
        wrow[k] = sums[0:1, k * 128 : (k + 1) * 128]

    def ring(a, major, minor):
        major, minor = lax.rem(major + 4, 4), lax.rem(minor + 4, 4)
        return device(major, e, minor) if a == 0 else device(minor, e, major)

    mine = ((y, x), (x, y))

    def share_ref(a, dmajor, dminor, first_block, blocks):
        major, minor = mine[a]
        share = lax.rem(major + dmajor + 4, 4) * 4 + lax.rem(minor + dminor + 4, 4)
        return full.at[a, share, pl.ds(first_block, blocks)]

    def major_ref(a, dmajor, first_block, blocks):
        share = lax.rem(mine[a][0] + dmajor + 4, 4) * 4
        return full.at[a, pl.ds(share, 4), pl.ds(first_block, blocks)]

    def send_group(g, a, tag, ref, dmajor, dminor):
        major, minor = mine[a]
        remote(ref, ref, g_send.at[g, a, tag], g_recv.at[g, a, tag], ring(a, major + dmajor, minor + dminor))

    def step_a(g):
        b, n = GROUPS[g]
        for a in range(2):
            for i in range(n):
                arrived(full.at[a, shares[a], b + i], z_recv.at[a, b + i])
            for tag, d in ((0, 1), (1, -1)):
                send_group(g, a, tag, share_ref(a, 0, 0, b, n), 0, d)

    def step_b(g):
        b, n = GROUPS[g]
        h = n // 2
        for a in range(2):
            arrived(share_ref(a, 0, -1, b, n), g_recv.at[g, a, 0])
            send_group(g, a, 2, share_ref(a, 0, -1, b, h), 0, 1)
            arrived(share_ref(a, 0, 1, b, n), g_recv.at[g, a, 1])
            send_group(g, a, 3, share_ref(a, 0, 1, b + h, h), 0, -1)

    def step_c(g):
        b, n = GROUPS[g]
        h = n // 2
        for a in range(2):
            arrived(share_ref(a, 0, 2, b, h), g_recv.at[g, a, 2])
            arrived(share_ref(a, 0, 2, b + h, h), g_recv.at[g, a, 3])
            for tag, d in ((4, 1), (5, -1)):
                send_group(g, a, tag, major_ref(a, 0, b, n), d, 0)

    def step_d(g):
        b, n = GROUPS[g]
        h = n // 2
        for a in range(2):
            arrived(major_ref(a, -1, b, n), g_recv.at[g, a, 4])
            send_group(g, a, 6, major_ref(a, -1, b, h), 1, 0)
            arrived(major_ref(a, 1, b, n), g_recv.at[g, a, 5])
            send_group(g, a, 7, major_ref(a, 1, b + h, h), -1, 0)

    def step_e(g):
        b, n = GROUPS[g]
        h = n // 2
        for a in range(2):
            arrived(major_ref(a, 2, b, h), g_recv.at[g, a, 6])
            arrived(major_ref(a, 2, b + h, h), g_recv.at[g, a, 7])

    def rows_of(a, chunk, b0):
        return jnp.concatenate([full[a, chunk * 4 + i, b0 : b0 + 8].reshape(256, COLS) for i in range(4)], axis=1)

    def chunk_in(cg, chunk, begin):
        ks = pl.ds(pl.multiple_of(chunk * 1024, 1024), 1024)
        rows = rows_of(0, chunk, cg * 8)
        for acc, w in ((acc0, wg), (acc1, wu)):
            v = nt(rows, w[:, ks])
            acc[...] = v if begin else acc[...] + v

    def chunk_back(cg, chunk, begin):
        ks = pl.ds(pl.multiple_of(chunk * 1024, 1024), 1024)
        v = nt(rows_of(1, chunk, cg * 8), wd[:, ks])
        acc2[...] = v if begin else acc2[...] + v

    def chunks(cg, offset, begin):
        chunk_in(cg, lax.rem(y + offset, 4), begin)
        chunk_back(cg, lax.rem(x + offset, 4), begin)

    def activations(cg):
        gate, up, back = acc0[:, :448], acc1[...], acc2[:, :448]
        s = jax.nn.sigmoid(gate)
        gated = gate * s
        hidden = (gated * up).astype(BF16)
        d_up = (back * gated).astype(BF16)
        d_gate = (back * up * s * (1.0 + gate * (1.0 - s))).astype(BF16)
        sums = nt(d_up, pbt1[...]) + nt(d_gate, pbt2[...]) + nt(hidden, pat[...])
        part[cg] = sums.astype(BF16).reshape(16, 16, 256)
        keep_in[cg] = acc0[:, 384:512]
        keep_out[cg] = acc2[:, 384:512]

    def scatter(cg):
        for r, (dy, dx) in enumerate(PLANE):
            remote(
                part.at[cg, plane_index(dy, dx)],
                gathered.at[cg, me],
                rs_send.at[cg, r],
                rs_recv.at[cg, r],
                plane(dy, dx),
            )

    def gather(cg):
        total = part[cg, me].astype(F32)
        for r, (dy, dx) in enumerate(PLANE):
            source = plane_index(4 - dy, 4 - dx)
            arrived(gathered.at[cg, source], rs_recv.at[cg, r])
            total = total + gathered[cg, source].astype(F32)
        own[cg] = total.astype(BF16)
        for r, (dy, dx) in enumerate(PLANE):
            remote(own.at[cg], factors.at[cg, me], ag_send.at[cg, r], ag_recv.at[cg, r], plane(dy, dx))
        factors[cg, me] = total.astype(BF16)

    low_half = iota((256, 128), 1) < 64
    pairs = iota((128, 256), 1) // 16 * 2

    def picked(shift, odd):
        return (iota((128, 256), 0) == pairs + (shift + odd)).astype(F32).astype(BF16)

    def spread(values, odd):
        high, low = split(values)
        return nn(high, picked(64, odd)) + nn(low, picked(64, odd))

    def against(values, w):
        high, low = split(values)
        return nt(high, w) + nt(low, w)

    def scores(cg):
        for r, (dy, dx) in enumerate(PLANE):
            arrived(factors.at[cg, plane_index(4 - dy, 4 - dx)], ag_recv.at[cg, r])
        all_rows = factors[cg].reshape(256, 256)
        b_both = all_rows[:, :128].astype(F32)
        b_turned = pltpu.roll(b_both, 64, 1)
        b_out = keep_out[cg]
        out_turned = pltpu.roll(b_out, 64, 1)
        a_hidden, a_in = all_rows[:, 128:], keep_in[cg]
        even = jnp.concatenate([jnp.where(low_half, b_both, 0.0), jnp.where(low_half, b_turned, 0.0)], axis=1)
        odd = jnp.concatenate([jnp.where(low_half, 0.0, b_turned), jnp.where(low_half, 0.0, b_both)], axis=1)
        z_sum = spread(a_in, 0) * nt(even.astype(BF16), wq12[...])
        z_sum += spread(a_in, 1) * nt(odd.astype(BF16), wq12[...])
        z_sum += nn(a_hidden, picked(0, 0)) * against(jnp.where(low_half, out_turned, 0.0), wq0[...])
        z_sum += nn(a_hidden, picked(0, 1)) * against(jnp.where(low_half, 0.0, b_out), wq0[...])
        high, low = split(z_sum)
        fold = (lax.rem(iota((16, 256), 1), 16) == iota((16, 256), 0)).astype(F32).astype(BF16)
        score = nt(fold, high) + nt(fold, low)
        for t in range(2):
            score_send[cg, t] = score[:, t * 128 : (t + 1) * 128]
        for pos in range(cg * 4, cg * 4 + 4):
            tile = score_send.at[cg, (pos % 4) // 2]
            for core in range(2):
                if pos != LOCAL:
                    remote(
                        tile,
                        score_recv.at[2 * pos + c],
                        sc_send.at[2 * pos + core],
                        sc_recv.at[2 * pos + c],
                        back_column(pos, core),
                    )
            if pos == LOCAL:
                remote(
                    tile,
                    score_recv.at[2 * pos + c],
                    sc_send.at[2 * pos],
                    sc_recv.at[2 * pos + c],
                    device(y, z * 2 + other, x),
                )
                score_recv[2 * pos + c] = score_send[cg, (pos % 4) // 2]
        share = jnp.zeros((16, 128), F32)
        for t in range(2):
            w_tile = jnp.zeros((1, 128), F32)
            for k in range(4):
                w_tile = w_tile + wrecv[cg * 8 + t * 4 + k]
            share = share + score[:, t * 128 : (t + 1) * 128] * w_tile
        return jnp.sum(share, axis=1, keepdims=True)

    def constants():
        wg[480:512] = jnp.zeros((32, 4096), BF16)
        loads["q"].wait()
        for i in range(16):
            wq0[i * 16 : (i + 1) * 16, :] = qs[:, i * 128 : (i + 1) * 128]
            wq12[i * 16 : (i + 1) * 16, 0:128] = qs[:, 2048 + i * 128 : 2048 + (i + 1) * 128]
            wq12[i * 16 : (i + 1) * 16, 128:256] = qs[:, 4096 + i * 128 : 4096 + (i + 1) * 128]
        loads["pa"].wait()
        loads["pb"].wait()
        at = iota((256, 64), 0) - iota((256, 64), 1)
        pbt1[...] = nn((at == 0).astype(F32).astype(BF16), pb[...]).astype(BF16)
        pbt2[...] = nn((at == 64).astype(F32).astype(BF16), pb[...]).astype(BF16)
        at = iota((256, 32), 0) - iota((256, 32), 1)
        pat[...] = nn((at == 128).astype(F32).astype(BF16), pa[...]).astype(BF16)

    def send_weights():
        for pos in range(NZ):
            if pos == LOCAL:
                remote(
                    wrow.at[2 * pos + other],
                    wrecv.at[2 * pos + c],
                    w_send.at[2 * pos],
                    w_recv.at[2 * pos + c],
                    device(y, z * 2 + other, x),
                )
                wrecv[2 * pos + c] = wrow[2 * pos + c]
            else:
                for core in range(2):
                    remote(
                        wrow.at[2 * pos + core],
                        wrecv.at[2 * pos + c],
                        w_send.at[2 * pos + core],
                        w_recv.at[2 * pos + c],
                        column(pos, core),
                    )

    step_a(0)
    step_b(0)
    step_a(1)
    step_c(0)
    step_b(1)
    step_a(2)
    send_weights()
    step_d(0)
    step_c(1)
    step_b(2)
    step_a(3)
    constants()
    step_e(0)
    step_d(1)
    step_c(2)
    step_b(3)
    for name in ("pin", "pout", "wg", "wu", "wd"):
        loads[name].wait()
    step_e(1)
    chunks(0, 0, True)
    for offset in (1, 2):
        chunks(0, offset, False)
    step_d(2)
    step_c(3)
    chunks(0, 3, False)
    activations(0)
    scatter(0)
    for pos in range(NZ):
        for core in range(2):
            if pos != LOCAL:
                arrived(wrecv.at[2 * pos + core], w_recv.at[2 * pos + core])
    arrived(wrecv.at[2 * LOCAL + other], w_recv.at[2 * LOCAL + other])
    for a in range(2):
        arrived(full.at[a, :, 2 * LOCAL + other], pair_recv.at[a])
    chunks(1, 0, True)
    step_d(3)
    gather(0)
    step_e(2)
    chunks(1, 1, False)
    chunks(1, 3, False)
    total0 = scores(0)
    step_e(3)
    chunks(1, 2, False)
    activations(1)
    scatter(1)
    gather(1)
    total = total0 + scores(1)

    on_diagonal = iota((16, 128), 0) == iota((16, 128), 1)
    row = jnp.sum(jnp.where(on_diagonal, total, 0.0), axis=0, keepdims=True)
    tot_send[...] = row
    tot_recv[2 * LOCAL + c] = row
    for pos in range(NZ):
        for core in range(2):
            if pos != LOCAL:
                k = 2 * pos + core
                remote(tot_send, tot_recv.at[2 * pos + c], t_send.at[k], t_recv.at[2 * pos + c], back_column(pos, core))
    remote(
        tot_send,
        tot_recv.at[2 * LOCAL + c],
        t_send.at[2 * LOCAL],
        t_recv.at[2 * LOCAL + c],
        device(y, z * 2 + other, x),
    )

    def wait_all(buffer, sems):
        for pos in range(NZ):
            for core in range(2):
                if pos != LOCAL:
                    arrived(buffer.at[2 * pos + core], sems.at[2 * pos + core])
        arrived(buffer.at[2 * LOCAL + other], sems.at[2 * LOCAL + other])

    wait_all(score_recv, sc_recv)
    every = jnp.concatenate([score_recv[k] for k in range(16)], axis=1)
    high, low = split(every)
    tok_ref[...] = nn(high, wm_hi[...]) + nn(high, wm_lo[...]) + nn(low, wm_hi[...])
    wait_all(tot_recv, t_recv)
    row = tot_recv[0]
    for k in range(1, 16):
        row = row + tot_recv[k]
    tot_ref[...] = row[:, :16] * (1.0 / math.sqrt(2048.0))
    for copy in sent:
        copy.wait_send()


def body(inputs, cotangents, routes, gates, w_gate, w_up, w_down, proj_in, proj_out, proj_hid_a, proj_hid_b, queries):
    anywhere = pl.BlockSpec(memory_space=pl.ANY)
    vmem = pl.BlockSpec(memory_space=pltpu.VMEM)
    scores, totals = pl.pallas_call(
        kernel,
        out_shape=(jax.ShapeDtypeStruct((16, 128), F32), jax.ShapeDtypeStruct((1, 16), F32)),
        in_specs=[anywhere] * 12,
        out_specs=(vmem, vmem),
        scratch_shapes=[
            pltpu.VMEM((128, 4096), BF16),
            pltpu.VMEM((128, 4096), BF16),
            pltpu.VMEM((2, 128), I32),
            pltpu.VMEM((2, 128), F32),
            pltpu.VMEM((512, 4096), BF16),
            pltpu.VMEM((448, 4096), BF16),
            pltpu.VMEM((512, 4096), BF16),
            pltpu.VMEM((32, 448), BF16),
            pltpu.VMEM((64, 448), BF16),
            pltpu.VMEM((16, 6144), BF16),
            pltpu.VMEM((2, SHARES, 16, SLOTS, COLS), BF16),
            pltpu.VMEM((2, 16, SLOTS, COLS), BF16),
            pltpu.VMEM((2, SHARES, SLOTS, COLS), BF16),
            pltpu.VMEM((256, 512), F32),
            pltpu.VMEM((256, 448), F32),
            pltpu.VMEM((256, 512), F32),
            pltpu.VMEM((2, 256, 128), F32),
            pltpu.VMEM((2, 256, 128), F32),
            pltpu.VMEM((256, 448), BF16),
            pltpu.VMEM((256, 448), BF16),
            pltpu.VMEM((256, 448), BF16),
            pltpu.VMEM((256, 128), BF16),
            pltpu.VMEM((256, 256), BF16),
            pltpu.VMEM((2048, 128), BF16),
            pltpu.VMEM((2048, 128), BF16),
            pltpu.VMEM((16, 1, 128), F32),
            pltpu.VMEM((16, 1, 128), F32),
            pltpu.VMEM((2, 16, 16, 256), BF16),
            pltpu.VMEM((2, 16, 16, 256), BF16),
            pltpu.VMEM((2, 16, 256), BF16),
            pltpu.VMEM((2, 16, 16, 256), BF16),
            pltpu.VMEM((2, 2, 16, 128), F32),
            pltpu.VMEM((16, 16, 128), F32),
            pltpu.VMEM((1, 128), F32),
            pltpu.VMEM((16, 1, 128), F32),
            pltpu.SemaphoreType.DMA((12,)),
            pltpu.SemaphoreType.DMA((2, 16)),
            pltpu.SemaphoreType.DMA((2, 16)),
            pltpu.SemaphoreType.DMA((2,)),
            pltpu.SemaphoreType.DMA((2,)),
            pltpu.SemaphoreType.DMA((16,)),
            pltpu.SemaphoreType.DMA((16,)),
            pltpu.SemaphoreType.DMA((4, 2, 8)),
            pltpu.SemaphoreType.DMA((4, 2, 8)),
            pltpu.SemaphoreType.DMA((2, 15)),
            pltpu.SemaphoreType.DMA((2, 15)),
            pltpu.SemaphoreType.DMA((2, 15)),
            pltpu.SemaphoreType.DMA((2, 15)),
            pltpu.SemaphoreType.DMA((16,)),
            pltpu.SemaphoreType.DMA((16,)),
            pltpu.SemaphoreType.DMA((16,)),
            pltpu.SemaphoreType.DMA((16,)),
        ],
        compiler_params=pltpu.CompilerParams(
            collective_id=0, has_side_effects=True, vmem_limit_bytes=60 * 1024 * 1024
        ),
    )(
        inputs,
        cotangents,
        routes.T,
        gates.T,
        w_gate[0].T,
        w_up[0].T,
        w_down[0],
        proj_in.T,
        proj_out.T,
        proj_hid_a.T,
        proj_hid_b.T,
        queries,
    )
    return scores.T, totals.reshape(16)


def solution(mesh):
    placed = (
        P("expert", None),
        P("expert", None),
        P("expert", None),
        P("expert", None),
        P("expert", None, ("dp", "pipe")),
        P("expert", None, ("dp", "pipe")),
        P("expert", ("dp", "pipe"), None),
        P(),
        P(),
        P(("dp", "pipe"), None),
        P(("dp", "pipe"), None),
        P(("dp", "pipe"), None),
    )
    return jax.shard_map(
        body,
        mesh=mesh,
        in_specs=placed,
        out_specs=(P("expert", ("dp", "pipe")), P(("dp", "pipe"))),
        check_vma=False,
    )
```

```python
import math

import jax
import jax.numpy as jnp
from jax import lax
from jax.experimental import pallas as pl
from jax.experimental.pallas import tpu as pltpu
from jax.sharding import PartitionSpec as P

MESH = pl.DeviceIdType.MESH
F32, BF16, I32 = jnp.float32, jnp.bfloat16, jnp.int32

NZ = 8
ORDER = (2, 6, 3, 5, 4, 0, 1, 7)
LOCAL = ORDER.index(0)
NEAR = 6
SLOTS = 32
COLS = 256
SHARES = 16
GROUPS = ((0, 4), (4, 4), (8, 2))
PIECES = (0, -1, 1, 2)
PLANE = sorted(
    ((dy, dx) for dy in range(4) for dx in range(4) if dy or dx),
    key=lambda o: min(o[0], 4 - o[0]) + min(o[1], 4 - o[1]),
)


def nn(a, b):
    return lax.dot_general(a, b, (((1,), (0,)), ((), ())), preferred_element_type=F32)


def nt(a, b):
    return lax.dot_general(a, b, (((1,), (1,)), ((), ())), preferred_element_type=F32)


def iota(shape, dim):
    return lax.broadcasted_iota(I32, shape, dim)


def split(v):
    high = v.astype(BF16)
    return high, (v - high.astype(F32)).astype(BF16)


def kernel(
    x_hbm, g_hbm, routes_hbm, gates_hbm, wg_hbm, wu_hbm, wd_hbm, pin_hbm, pout_hbm, pa_hbm, pb_hbm, q_hbm,
    tok_ref, tot_ref,
    xs, gs, routes, gates, wg, wu, wd, pa, pb, qs,
    full, out_rows, out_pair, out_near, acc0, acc1, acc2, terms,
    pat, pbt1, pbt2, wq0, wq12, wm_hi, wm_lo, wrow, wrecv,
    part, gathered, own, factors, score_send, score_recv, tot_send, tot_recv,
    load_sem, z_send, z_recv, pair_recv, near_recv, w_send, w_recv,
    g_send, g_recv, e_recv, rs_send, rs_recv, ag_send, ag_recv, sc_send, sc_recv, t_send, t_recv,
):
    y, e, x = lax.axis_index("dp"), lax.axis_index("expert"), lax.axis_index("pipe")
    z, c = lax.div(e, 2), lax.rem(e, 2)
    other = 1 - c
    me = y * 4 + x

    def device(yy, ee, xx):
        return {"dp": yy, "expert": ee, "pipe": xx}

    def column(pos, core):
        return device(y, lax.rem(z + ORDER[pos], NZ) * 2 + core, x)

    def back_column(pos, core):
        return device(y, lax.rem(z + NZ - ORDER[pos], NZ) * 2 + core, x)

    def plane(dy, dx):
        return device(lax.rem(y + dy, 4), e, lax.rem(x + dx, 4))

    def plane_index(dy, dx):
        return lax.rem(y + dy, 4) * 4 + lax.rem(x + dx, 4)

    def remote(src, dst, ss, rs, dev):
        pltpu.make_async_remote_copy(
            src_ref=src, dst_ref=dst, send_sem=ss, recv_sem=rs, device_id=dev, device_id_type=MESH
        ).start()

    def arrived(dst, rs):
        pltpu.make_async_remote_copy(
            src_ref=dst, dst_ref=dst, send_sem=rs, recv_sem=rs, device_id=device(y, e, x), device_id_type=MESH
        ).wait_recv()

    def left(src, ss):
        pltpu.make_async_remote_copy(
            src_ref=src, dst_ref=src, send_sem=ss, recv_sem=ss, device_id=device(y, e, x), device_id_type=MESH
        ).wait_send()

    barrier = pltpu.get_barrier_semaphore()
    for dy, dx in PLANE:
        pl.semaphore_signal(barrier, inc=1, device_id=plane(dy, dx), device_id_type=MESH)
    for pos in range(NZ):
        if pos == LOCAL:
            pl.semaphore_signal(barrier, inc=1, device_id=column(pos, other), device_id_type=MESH)
        else:
            for core in range(2):
                pl.semaphore_signal(barrier, inc=1, device_id=column(pos, core), device_id_type=MESH)

    loads = {}
    for i, (name, src, dst) in enumerate(
        (
            ("routes", routes_hbm, routes),
            ("gates", gates_hbm, gates),
            ("x", x_hbm, xs),
            ("g", g_hbm, gs),
            ("q", q_hbm, qs),
            ("pa", pa_hbm, pa),
            ("pb", pb_hbm, pb),
            ("pin", pin_hbm, wg.at[448:480]),
            ("pout", pout_hbm, wd.at[448:512]),
            ("wg", wg_hbm, wg.at[0:448]),
            ("wu", wu_hbm, wu),
            ("wd", wd_hbm, wd.at[0:448]),
        )
    ):
        loads[name] = pltpu.make_async_copy(src, dst, load_sem.at[i])
        loads[name].start()

    loads["routes"].wait()
    loads["gates"].wait()
    first, second = routes[0:1, :], routes[1:2, :]
    expert_rows = iota((16, 128), 0)
    named = ((expert_rows == first) | (expert_rows == second)).astype(F32)
    before = (iota((128, 128), 0) < iota((128, 128), 1)).astype(F32)
    earlier = nn(named.astype(BF16), before.astype(BF16))

    def places(route):
        slot = jnp.sum(jnp.where(expert_rows == route, earlier, 0.0), axis=0, keepdims=True).astype(I32)
        offset = ((route >> 1) - z) & (NZ - 1)
        pos = jnp.zeros_like(offset)
        for i, o in enumerate(ORDER):
            pos = jnp.where(offset == o, i, pos)
        block = pos * 2 + (route & 1)
        lane = block * 128 + ((pos & 1) * 2 + c) * 32 + slot
        return block * SLOTS + slot, lane

    place0, lane0 = places(first)
    place1, lane1 = places(second)

    def picks_of(start, count):
        rows = iota((count, 128), 0) + start
        return ((rows == place0) | (rows == place1)).astype(F32).astype(BF16)

    far = 10 * SLOTS
    picks = picks_of(0, far)
    shares = (y * 4 + x, x * 4 + y)
    for a, (name, source) in enumerate((("x", xs), ("g", gs))):
        loads[name].wait()
        columns = pl.ds(pl.multiple_of(shares[a] * COLS, COLS), COLS)
        rows = nn(picks, source[:, columns]).astype(BF16)
        out_rows[a] = rows.reshape(10, SLOTS, COLS)

    pl.semaphore_wait(barrier, 30)

    def send_far(*positions):
        for pos in positions:
            for a in range(2):
                for core in range(2):
                    remote(
                        out_rows.at[a, 2 * pos + core],
                        full.at[a, shares[a], 2 * pos + c],
                        z_send,
                        z_recv.at[pos // 2, a],
                        column(pos, core),
                    )

    send_far(0, 1)

    near_picks = picks_of(2 * NEAR * SLOTS, 4 * SLOTS)
    for a, source in enumerate((xs, gs)):
        for p in range(SHARES):
            rows = nn(near_picks, source[:, p * COLS : (p + 1) * COLS]).astype(BF16)
            out_near[a, :, p] = rows.reshape(4, SLOTS, COLS)

    def send_near():
        for a in range(2):
            for core in range(2):
                for pos in range(NEAR, NZ):
                    k = 2 * (pos - NEAR)
                    remote(
                        out_near.at[a, k + core],
                        full.at[a, :, 2 * pos + c],
                        z_send,
                        near_recv,
                        column(pos, core),
                    )

    def chip_rows():
        pair_picks = picks_of((2 * LOCAL + other) * SLOTS, SLOTS)
        own_picks = picks_of((2 * LOCAL + c) * SLOTS, SLOTS)
        for a, source in enumerate((xs, gs)):
            for p in range(SHARES):
                columns = source[:, p * COLS : (p + 1) * COLS]
                out_pair[a, p] = nn(pair_picks, columns).astype(BF16)
                full[a, p, 2 * LOCAL + c] = nn(own_picks, columns).astype(BF16)

    def send_pair():
        for a in range(2):
            remote(
                out_pair.at[a],
                full.at[a, :, 2 * LOCAL + c],
                z_send,
                pair_recv,
                device(y, z * 2 + other, x),
            )

    def slot_weights():
        lanes = iota((2048, 128), 0)
        weights = jnp.where(lanes == lane0, gates[0:1, :], 0.0) + jnp.where(lanes == lane1, gates[1:2, :], 0.0)
        high, low = split(weights)
        wm_hi[...] = high
        wm_lo[...] = low
        ones = jnp.ones((8, 128), BF16)
        sums = nt(ones, high) + nt(ones, low)
        for k in range(16):
            wrow[k] = sums[0:1, k * 128 : (k + 1) * 128]

    def ring(a, major, minor):
        major, minor = lax.rem(major + 4, 4), lax.rem(minor + 4, 4)
        return device(major, e, minor) if a == 0 else device(minor, e, major)

    mine = ((y, x), (x, y))

    def share_ref(a, dmajor, dminor, first_block, blocks):
        major, minor = mine[a]
        share = lax.rem(major + dmajor + 4, 4) * 4 + lax.rem(minor + dminor + 4, 4)
        return full.at[a, share, pl.ds(first_block, blocks)]

    def send_group(a, ref, sem, dmajor, dminor):
        major, minor = mine[a]
        remote(ref, ref, g_send, sem, ring(a, major + dmajor, minor + dminor))

    def send_piece(g, a, piece):
        b, n = GROUPS[g]
        for way, d in enumerate((1, -1)):
            send_group(a, share_ref(a, 0, PIECES[piece], b, n), g_recv.at[g, a, 3 + 2 * piece + way], d, 0)

    def step_a(g):
        b, n = GROUPS[g]
        for a in range(2):
            arrived(share_ref(a, 0, 0, b, n), z_recv.at[g, a])
            for tag, d in ((0, 1), (1, -1)):
                send_group(a, share_ref(a, 0, 0, b, n), g_recv.at[g, a, tag], 0, d)
        if g == 0:
            for a in range(2):
                send_piece(g, a, 0)

    def step_b(g):
        b, n = GROUPS[g]
        h = n // 2
        for a in range(2):
            arrived(share_ref(a, 0, -1, b, n), g_recv.at[g, a, 0])
            send_group(a, share_ref(a, 0, -1, b, h), g_recv.at[g, a, 2], 0, 1)
            arrived(share_ref(a, 0, 1, b, n), g_recv.at[g, a, 1])
            send_group(a, share_ref(a, 0, 1, b + h, h), g_recv.at[g, a, 2], 0, -1)
        for a in range(2):
            for piece in (1, 2) if g == 0 else (0, 1, 2):
                send_piece(g, a, piece)

    def step_c(g):
        b, n = GROUPS[g]
        for a in range(2):
            arrived(share_ref(a, 0, 2, b, n), g_recv.at[g, a, 2])
            send_piece(g, a, 3)

    def step_d(g, *pieces):
        b, n = GROUPS[g]
        h = n // 2
        for piece in pieces:
            dm, tag = PIECES[piece], 3 + 2 * piece
            for a in range(2):
                arrived(share_ref(a, -1, dm, b, n), g_recv.at[g, a, tag])
                send_group(a, share_ref(a, -1, dm, b, h), e_recv.at[g], 1, 0)
                arrived(share_ref(a, 1, dm, b, n), g_recv.at[g, a, tag + 1])
                send_group(a, share_ref(a, 1, dm, b + h, h), e_recv.at[g], -1, 0)

    def step_e(g):
        b, n = GROUPS[g]
        arrived(full.at[:, 0:4, pl.ds(b, n)], e_recv.at[g])

    def rows_of(a, chunk, b0):
        return jnp.concatenate([full[a, chunk * 4 + i, b0 : b0 + 8].reshape(256, COLS) for i in range(4)], axis=1)

    def chunk_in(cg, chunk, begin):
        ks = pl.ds(pl.multiple_of(chunk * 1024, 1024), 1024)
        rows = rows_of(0, chunk, cg * 8)
        for acc, w in ((acc0, wg), (acc1, wu)):
            v = nt(rows, w[:, ks])
            acc[cg] = v if begin else acc[cg] + v

    def chunk_back(cg, chunk, begin):
        ks = pl.ds(pl.multiple_of(chunk * 1024, 1024), 1024)
        v = nt(rows_of(1, chunk, cg * 8), wd[:, ks])
        acc2[cg] = v if begin else acc2[cg] + v

    def chunks(cg, offset, begin):
        chunk_in(cg, lax.rem(y + offset, 4), begin)
        chunk_back(cg, lax.rem(x + offset, 4), begin)

    def activations(cg):
        gate, up, back = acc0[cg, :, :448], acc1[cg], acc2[cg, :, :448]
        s = jax.nn.sigmoid(gate)
        gated = gate * s
        hidden = (gated * up).astype(BF16)
        d_up = (back * gated).astype(BF16)
        d_gate = (back * up * s * (1.0 + gate * (1.0 - s))).astype(BF16)
        sums = nt(d_up, pbt1[...]) + nt(d_gate, pbt2[...]) + nt(hidden, pat[...])
        part[cg] = sums.astype(BF16).reshape(16, 16, 256)

    def scatter(cg):
        for dy, dx in PLANE:
            remote(
                part.at[cg, plane_index(dy, dx)],
                gathered.at[cg, me],
                rs_send.at[cg],
                rs_recv.at[cg],
                plane(dy, dx),
            )

    def gather(cg):
        total = part[cg, me].astype(F32)
        arrived(gathered.at[cg, 0:15], rs_recv.at[cg])
        for dy, dx in PLANE:
            total = total + gathered[cg, plane_index(dy, dx)].astype(F32)
        own[cg] = total.astype(BF16)
        for dy, dx in PLANE:
            remote(own.at[cg], factors.at[cg, me], ag_send.at[cg], ag_recv.at[cg], plane(dy, dx))
        factors[cg, me] = total.astype(BF16)

    low_half = iota((256, 128), 1) < 64
    pairs = iota((128, 256), 1) // 16 * 2

    def picked(shift, odd):
        return (iota((128, 256), 0) == pairs + (shift + odd)).astype(F32).astype(BF16)

    def spread(values, odd):
        high, low = split(values)
        return nn(high, picked(64, odd)) + nn(low, picked(64, odd))

    def against(values, w):
        high, low = split(values)
        return nt(high, w) + nt(low, w)

    def local_terms(cg):
        a_in, b_out = acc0[cg, :, 384:512], acc2[cg, :, 384:512]
        out_turned = pltpu.roll(b_out, 64, 1)
        terms[cg, 0] = spread(a_in, 0)
        terms[cg, 1] = spread(a_in, 1)
        terms[cg, 2] = against(jnp.where(low_half, out_turned, 0.0), wq0[...])
        terms[cg, 3] = against(jnp.where(low_half, 0.0, b_out), wq0[...])

    def scores(cg):
        arrived(factors.at[cg, 0:15], ag_recv.at[cg])
        all_rows = factors[cg].reshape(256, 256)
        b_both = all_rows[:, :128].astype(F32)
        b_turned = pltpu.roll(b_both, 64, 1)
        a_hidden = all_rows[:, 128:]
        even = jnp.concatenate([jnp.where(low_half, b_both, 0.0), jnp.where(low_half, b_turned, 0.0)], axis=1)
        odd = jnp.concatenate([jnp.where(low_half, 0.0, b_turned), jnp.where(low_half, 0.0, b_both)], axis=1)
        z_sum = terms[cg, 0] * nt(even.astype(BF16), wq12[...])
        z_sum += terms[cg, 1] * nt(odd.astype(BF16), wq12[...])
        z_sum += nn(a_hidden, picked(0, 0)) * terms[cg, 2]
        z_sum += nn(a_hidden, picked(0, 1)) * terms[cg, 3]
        high, low = split(z_sum)
        fold = (lax.rem(iota((16, 256), 1), 16) == iota((16, 256), 0)).astype(F32).astype(BF16)
        score = nt(fold, high) + nt(fold, low)
        for t in range(2):
            score_send[cg, t] = score[:, t * 128 : (t + 1) * 128]
        for pos in range(cg * 4, cg * 4 + 4):
            tile = score_send.at[cg, (pos % 4) // 2]
            for core in range(2):
                if pos != LOCAL:
                    remote(
                        tile,
                        score_recv.at[2 * pos + c],
                        sc_send,
                        sc_recv,
                        back_column(pos, core),
                    )
            if pos == LOCAL:
                remote(
                    tile,
                    score_recv.at[2 * pos + c],
                    sc_send,
                    sc_recv,
                    device(y, z * 2 + other, x),
                )
                score_recv[2 * pos + c] = score_send[cg, (pos % 4) // 2]
        share = jnp.zeros((16, 128), F32)
        for t in range(2):
            w_tile = jnp.zeros((1, 128), F32)
            for k in range(4):
                w_tile = w_tile + wrecv[cg * 8 + t * 4 + k]
            share = share + score[:, t * 128 : (t + 1) * 128] * w_tile
        return jnp.sum(share, axis=1, keepdims=True)

    def constants():
        wg[480:512] = jnp.zeros((32, 4096), BF16)
        loads["q"].wait()
        for i in range(16):
            wq0[i * 16 : (i + 1) * 16, :] = qs[:, i * 128 : (i + 1) * 128]
            wq12[i * 16 : (i + 1) * 16, 0:128] = qs[:, 2048 + i * 128 : 2048 + (i + 1) * 128]
            wq12[i * 16 : (i + 1) * 16, 128:256] = qs[:, 4096 + i * 128 : 4096 + (i + 1) * 128]
        loads["pa"].wait()
        loads["pb"].wait()
        at = iota((256, 64), 0) - iota((256, 64), 1)
        pbt1[...] = nn((at == 0).astype(F32).astype(BF16), pb[...]).astype(BF16)
        pbt2[...] = nn((at == 64).astype(F32).astype(BF16), pb[...]).astype(BF16)
        at = iota((256, 32), 0) - iota((256, 32), 1)
        pat[...] = nn((at == 128).astype(F32).astype(BF16), pa[...]).astype(BF16)

    def send_weights():
        for pos in range(NZ):
            if pos == LOCAL:
                remote(
                    wrow.at[2 * pos + other],
                    wrecv.at[2 * pos + c],
                    w_send,
                    w_recv,
                    device(y, z * 2 + other, x),
                )
                wrecv[2 * pos + c] = wrow[2 * pos + c]
            else:
                for core in range(2):
                    remote(
                        wrow.at[2 * pos + core],
                        wrecv.at[2 * pos + c],
                        w_send,
                        w_recv,
                        column(pos, core),
                    )

    chip_rows()
    slot_weights()
    send_far(2, 3)
    step_a(0)
    send_far(4)
    send_pair()
    send_near()
    send_weights()
    constants()
    step_b(0)
    step_a(1)
    step_c(0)
    step_d(0, 0)
    step_a(2)
    step_b(1)
    step_d(0, 1, 2)
    step_c(1)
    step_d(0, 3)
    step_b(2)
    for name in ("pin", "pout", "wg", "wu", "wd"):
        loads[name].wait()
    chunks(0, 0, True)
    step_d(1, 0)
    step_d(1, 1, 2)
    step_d(1, 3)
    chunks(0, 1, False)
    step_c(2)
    step_d(2, 0)
    chunks(0, 3, False)
    step_d(2, 1, 2)
    step_d(2, 3)
    step_e(0)
    step_e(1)
    chunks(0, 2, False)
    activations(0)
    scatter(0)
    arrived(full.at[:, :, 2 * NEAR : 2 * NEAR + 4], near_recv)
    arrived(full.at[:, :, 2 * LOCAL + other], pair_recv)
    chunks(1, 0, True)
    chunks(1, 1, False)
    chunks(1, 3, False)
    step_e(2)
    chunks(1, 2, False)
    activations(1)
    scatter(1)
    arrived(wrecv.at[0:15], w_recv)
    local_terms(0)
    gather(0)
    local_terms(1)
    gather(1)
    total0 = scores(0)
    total = total0 + scores(1)

    on_diagonal = iota((16, 128), 0) == iota((16, 128), 1)
    row = jnp.sum(jnp.where(on_diagonal, total, 0.0), axis=0, keepdims=True)
    tot_send[...] = row
    tot_recv[2 * LOCAL + c] = row
    for pos in range(NZ):
        for core in range(2):
            if pos != LOCAL:
                remote(tot_send, tot_recv.at[2 * pos + c], t_send, t_recv, back_column(pos, core))
    remote(
        tot_send,
        tot_recv.at[2 * LOCAL + c],
        t_send,
        t_recv,
        device(y, z * 2 + other, x),
    )

    arrived(score_recv.at[0:15], sc_recv)
    every = jnp.concatenate([score_recv[k] for k in range(16)], axis=1)
    high, low = split(every)
    tok_ref[...] = nn(high, wm_hi[...]) + nn(high, wm_lo[...]) + nn(low, wm_hi[...])
    arrived(tot_recv.at[0:15], t_recv)
    row = tot_recv[0]
    for k in range(1, 16):
        row = row + tot_recv[k]
    tot_ref[...] = row[:, :16] * (1.0 / math.sqrt(2048.0))
    left(full.at[:, 0:9, 0:10], z_send)
    left(full.at[:, 0:15, 0:10], g_send)
    left(wrecv.at[0:15], w_send)
    for cg in range(2):
        left(part.at[cg, 0:15], rs_send.at[cg])
        left(factors.at[cg, 0:15], ag_send.at[cg])
    left(score_recv.at[0:15], sc_send)
    left(tot_recv.at[0:15], t_send)


def body(inputs, cotangents, routes, gates, w_gate, w_up, w_down, proj_in, proj_out, proj_hid_a, proj_hid_b, queries):
    anywhere = pl.BlockSpec(memory_space=pl.ANY)
    vmem = pl.BlockSpec(memory_space=pltpu.VMEM)
    scores, totals = pl.pallas_call(
        kernel,
        out_shape=(jax.ShapeDtypeStruct((16, 128), F32), jax.ShapeDtypeStruct((1, 16), F32)),
        in_specs=[anywhere] * 12,
        out_specs=(vmem, vmem),
        scratch_shapes=[
            pltpu.VMEM((128, 4096), BF16),
            pltpu.VMEM((128, 4096), BF16),
            pltpu.VMEM((2, 128), I32),
            pltpu.VMEM((2, 128), F32),
            pltpu.VMEM((512, 4096), BF16),
            pltpu.VMEM((448, 4096), BF16),
            pltpu.VMEM((512, 4096), BF16),
            pltpu.VMEM((32, 448), BF16),
            pltpu.VMEM((64, 448), BF16),
            pltpu.VMEM((16, 6144), BF16),
            pltpu.VMEM((2, SHARES, 16, SLOTS, COLS), BF16),
            pltpu.VMEM((2, 10, SLOTS, COLS), BF16),
            pltpu.VMEM((2, SHARES, SLOTS, COLS), BF16),
            pltpu.VMEM((2, 4, SHARES, SLOTS, COLS), BF16),
            pltpu.VMEM((2, 256, 512), F32),
            pltpu.VMEM((2, 256, 448), F32),
            pltpu.VMEM((2, 256, 512), F32),
            pltpu.VMEM((2, 4, 256, 256), F32),
            pltpu.VMEM((256, 448), BF16),
            pltpu.VMEM((256, 448), BF16),
            pltpu.VMEM((256, 448), BF16),
            pltpu.VMEM((256, 128), BF16),
            pltpu.VMEM((256, 256), BF16),
            pltpu.VMEM((2048, 128), BF16),
            pltpu.VMEM((2048, 128), BF16),
            pltpu.VMEM((16, 1, 128), F32),
            pltpu.VMEM((16, 1, 128), F32),
            pltpu.VMEM((2, 16, 16, 256), BF16),
            pltpu.VMEM((2, 16, 16, 256), BF16),
            pltpu.VMEM((2, 16, 256), BF16),
            pltpu.VMEM((2, 16, 16, 256), BF16),
            pltpu.VMEM((2, 2, 16, 128), F32),
            pltpu.VMEM((16, 16, 128), F32),
            pltpu.VMEM((1, 128), F32),
            pltpu.VMEM((16, 1, 128), F32),
            pltpu.SemaphoreType.DMA((12,)),
            pltpu.SemaphoreType.DMA,
            pltpu.SemaphoreType.DMA((3, 2)),
            pltpu.SemaphoreType.DMA,
            pltpu.SemaphoreType.DMA,
            pltpu.SemaphoreType.DMA,
            pltpu.SemaphoreType.DMA,
            pltpu.SemaphoreType.DMA,
            pltpu.SemaphoreType.DMA((3, 2, 11)),
            pltpu.SemaphoreType.DMA((3,)),
            pltpu.SemaphoreType.DMA((2,)),
            pltpu.SemaphoreType.DMA((2,)),
            pltpu.SemaphoreType.DMA((2,)),
            pltpu.SemaphoreType.DMA((2,)),
            pltpu.SemaphoreType.DMA,
            pltpu.SemaphoreType.DMA,
            pltpu.SemaphoreType.DMA,
            pltpu.SemaphoreType.DMA,
        ],
        compiler_params=pltpu.CompilerParams(
            collective_id=0, has_side_effects=True, vmem_limit_bytes=60 * 1024 * 1024
        ),
    )(
        inputs,
        cotangents,
        routes.T,
        gates.T,
        w_gate[0].T,
        w_up[0].T,
        w_down[0],
        proj_in.T,
        proj_out.T,
        proj_hid_a.T,
        proj_hid_b.T,
        queries,
    )
    return scores.T, totals.reshape(16)


def solution(mesh):
    placed = (
        P("expert", None),
        P("expert", None),
        P("expert", None),
        P("expert", None),
        P("expert", None, ("dp", "pipe")),
        P("expert", None, ("dp", "pipe")),
        P("expert", ("dp", "pipe"), None),
        P(),
        P(),
        P(("dp", "pipe"), None),
        P(("dp", "pipe"), None),
        P(("dp", "pipe"), None),
    )
    return jax.shard_map(
        body,
        mesh=mesh,
        in_specs=placed,
        out_specs=(P("expert", ("dp", "pipe")), P(("dp", "pipe"))),
        check_vma=False,
    )
```

```python
import math

import jax
import jax.numpy as jnp
from jax import lax
from jax.experimental import pallas as pl
from jax.experimental.pallas import tpu as pltpu
from jax.sharding import PartitionSpec as P

MESH = pl.DeviceIdType.MESH
F32, BF16, I32 = jnp.float32, jnp.bfloat16, jnp.int32

NZ = 8
ORDER = (2, 6, 3, 5, 4, 0, 1, 7)
LOCAL = ORDER.index(0)
FIRST = (0, 1, 2, 3, LOCAL, 6, 7)
NEAR = 6
SLOTS = 32
COLS = 256
SHARES = 16
GROUPS = ((0, 4), (4, 4), (8, 2))
PIECES = (0, -1, 1, 2)
PLANE = sorted(
    ((dy, dx) for dy in range(4) for dx in range(4) if dy or dx),
    key=lambda o: -min(o[0], 4 - o[0]) - min(o[1], 4 - o[1]),
)
FAR_FIRST = sorted(range(NZ), key=lambda i: -min(ORDER[i], NZ - ORDER[i]))


def nn(a, b):
    return lax.dot_general(a, b, (((1,), (0,)), ((), ())), preferred_element_type=F32)


def nt(a, b):
    return lax.dot_general(a, b, (((1,), (1,)), ((), ())), preferred_element_type=F32)


def iota(shape, dim):
    return lax.broadcasted_iota(I32, shape, dim)


def split(v):
    high = v.astype(BF16)
    return high, (v - high.astype(F32)).astype(BF16)


def kernel(
    x_hbm, g_hbm, routes_hbm, gates_hbm, wg_hbm, wu_hbm, wd_hbm, pin_hbm, pout_hbm, pa_hbm, pb_hbm, q_hbm,
    tok_ref, tot_ref,
    xs, gs, routes, gates, wg, wu, wd, pa, pb, qs,
    full, out_rows, out_pair, out_near, acc0, acc1, acc2, terms,
    pat, pbt1, pbt2, wq0, wq12, wm_hi, wm_lo, wrow, wrecv,
    part, gathered, own, factors, score_send, score_recv, tot_send, tot_recv,
    load_sem, z_send, z_recv, pair_recv, near_recv, w_send, w_recv,
    g_send, g_recv, e_recv, rs_send, rs_recv, ag_send, ag_recv, sc_send, sc_recv, t_send, t_recv,
):
    y, e, x = lax.axis_index("dp"), lax.axis_index("expert"), lax.axis_index("pipe")
    z, c = lax.div(e, 2), lax.rem(e, 2)
    other = 1 - c
    me = y * 4 + x

    def device(yy, ee, xx):
        return {"dp": yy, "expert": ee, "pipe": xx}

    def column(pos, core):
        return device(y, lax.rem(z + ORDER[pos], NZ) * 2 + core, x)

    def back_column(pos, core):
        return device(y, lax.rem(z + NZ - ORDER[pos], NZ) * 2 + core, x)

    def plane(dy, dx):
        return device(lax.rem(y + dy, 4), e, lax.rem(x + dx, 4))

    def plane_index(dy, dx):
        return lax.rem(y + dy, 4) * 4 + lax.rem(x + dx, 4)

    def remote(src, dst, ss, rs, dev):
        pltpu.make_async_remote_copy(
            src_ref=src, dst_ref=dst, send_sem=ss, recv_sem=rs, device_id=dev, device_id_type=MESH
        ).start()

    def arrived(dst, rs):
        pltpu.make_async_remote_copy(
            src_ref=dst, dst_ref=dst, send_sem=rs, recv_sem=rs, device_id=device(y, e, x), device_id_type=MESH
        ).wait_recv()

    def left(src, ss):
        pltpu.make_async_remote_copy(
            src_ref=src, dst_ref=src, send_sem=ss, recv_sem=ss, device_id=device(y, e, x), device_id_type=MESH
        ).wait_send()

    barrier = pltpu.get_barrier_semaphore()
    for dy, dx in ((0, 1), (0, 3), (1, 0), (3, 0)):
        pl.semaphore_signal(barrier, inc=1, device_id=plane(dy, dx), device_id_type=MESH)
    for pos in FIRST:
        if pos == LOCAL:
            pl.semaphore_signal(barrier, inc=1, device_id=column(pos, other), device_id_type=MESH)
        else:
            for core in range(2):
                pl.semaphore_signal(barrier, inc=1, device_id=column(pos, core), device_id_type=MESH)

    loads = {}
    for i, (name, src, dst) in enumerate(
        (
            ("routes", routes_hbm, routes),
            ("gates", gates_hbm, gates),
            ("x", x_hbm, xs),
            ("g", g_hbm, gs),
            ("q", q_hbm, qs),
            ("pa", pa_hbm, pa),
            ("pb", pb_hbm, pb),
            ("pin", pin_hbm, wg.at[448:480]),
            ("pout", pout_hbm, wd.at[448:512]),
            ("wg", wg_hbm, wg.at[0:448]),
            ("wu", wu_hbm, wu),
            ("wd", wd_hbm, wd.at[0:448]),
        )
    ):
        loads[name] = pltpu.make_async_copy(src, dst, load_sem.at[i])
        loads[name].start()

    loads["routes"].wait()
    loads["gates"].wait()
    first, second = routes[0:1, :], routes[1:2, :]
    expert_rows = iota((16, 128), 0)
    named = ((expert_rows == first) | (expert_rows == second)).astype(F32)
    before = (iota((128, 128), 0) < iota((128, 128), 1)).astype(F32)
    earlier = nn(named.astype(BF16), before.astype(BF16))

    def places(route):
        slot = jnp.sum(jnp.where(expert_rows == route, earlier, 0.0), axis=0, keepdims=True).astype(I32)
        offset = ((route >> 1) - z) & (NZ - 1)
        pos = jnp.zeros_like(offset)
        for i, o in enumerate(ORDER):
            pos = jnp.where(offset == o, i, pos)
        block = pos * 2 + (route & 1)
        lane = block * 128 + ((pos & 1) * 2 + c) * 32 + slot
        return block * SLOTS + slot, lane

    place0, lane0 = places(first)
    place1, lane1 = places(second)

    def picks_of(start, count):
        rows = iota((count, 128), 0) + start
        return ((rows == place0) | (rows == place1)).astype(F32).astype(BF16)

    far = 10 * SLOTS
    picks = picks_of(0, far)
    shares = (y * 4 + x, x * 4 + y)
    for a, (name, source) in enumerate((("x", xs), ("g", gs))):
        loads[name].wait()
        columns = pl.ds(pl.multiple_of(shares[a] * COLS, COLS), COLS)
        rows = nn(picks, source[:, columns]).astype(BF16)
        out_rows[a] = rows.reshape(10, SLOTS, COLS)

    pl.semaphore_wait(barrier, 17)

    def send_far(*positions):
        for pos in positions:
            for a in range(2):
                for core in range(2):
                    remote(
                        out_rows.at[a, 2 * pos + core],
                        full.at[a, shares[a], 2 * pos + c],
                        z_send,
                        z_recv.at[pos // 2, a],
                        column(pos, core),
                    )

    send_far(0, 1)

    near_picks = picks_of(2 * NEAR * SLOTS, 4 * SLOTS)
    for a, source in enumerate((xs, gs)):
        for p in range(SHARES):
            rows = nn(near_picks, source[:, p * COLS : (p + 1) * COLS]).astype(BF16)
            out_near[a, :, p] = rows.reshape(4, SLOTS, COLS)

    def send_near():
        for a in range(2):
            for core in range(2):
                for pos in range(NEAR, NZ):
                    k = 2 * (pos - NEAR)
                    remote(
                        out_near.at[a, k + core],
                        full.at[a, :, 2 * pos + c],
                        z_send,
                        near_recv,
                        column(pos, core),
                    )

    def chip_rows():
        pair_picks = picks_of((2 * LOCAL + other) * SLOTS, SLOTS)
        own_picks = picks_of((2 * LOCAL + c) * SLOTS, SLOTS)
        for a, source in enumerate((xs, gs)):
            for p in range(SHARES):
                columns = source[:, p * COLS : (p + 1) * COLS]
                out_pair[a, p] = nn(pair_picks, columns).astype(BF16)
                full[a, p, 2 * LOCAL + c] = nn(own_picks, columns).astype(BF16)

    def send_pair():
        for a in range(2):
            remote(
                out_pair.at[a],
                full.at[a, :, 2 * LOCAL + c],
                z_send,
                pair_recv,
                device(y, z * 2 + other, x),
            )

    def slot_weights():
        lanes = iota((2048, 128), 0)
        weights = jnp.where(lanes == lane0, gates[0:1, :], 0.0) + jnp.where(lanes == lane1, gates[1:2, :], 0.0)
        high, low = split(weights)
        wm_hi[...] = high
        wm_lo[...] = low
        ones = jnp.ones((8, 128), BF16)
        sums = nt(ones, high) + nt(ones, low)
        for k in range(16):
            wrow[k] = sums[0:1, k * 128 : (k + 1) * 128]

    def ring(a, major, minor):
        major, minor = lax.rem(major + 4, 4), lax.rem(minor + 4, 4)
        return device(major, e, minor) if a == 0 else device(minor, e, major)

    mine = ((y, x), (x, y))

    def share_ref(a, dmajor, dminor, first_block, blocks):
        major, minor = mine[a]
        share = lax.rem(major + dmajor + 4, 4) * 4 + lax.rem(minor + dminor + 4, 4)
        return full.at[a, share, pl.ds(first_block, blocks)]

    def send_group(a, ref, sem, dmajor, dminor):
        major, minor = mine[a]
        remote(ref, ref, g_send, sem, ring(a, major + dmajor, minor + dminor))

    def send_piece(g, a, piece):
        b, n = GROUPS[g]
        for way, d in enumerate((1, -1)):
            send_group(a, share_ref(a, 0, PIECES[piece], b, n), g_recv.at[g, a, 3 + 2 * piece + way], d, 0)

    def step_a(g):
        b, n = GROUPS[g]
        h = n // 2
        for a in range(2):
            arrived(share_ref(a, 0, 0, b, n), z_recv.at[g, a])
            for tag, first in ((0, b), (1, b + h)):
                other_half = b + h if tag == 0 else b
                d = 1 if tag == 0 else -1
                send_group(a, share_ref(a, 0, 0, first, h), g_recv.at[g, a, tag], 0, d)
                send_group(a, share_ref(a, 0, 0, other_half, h), g_recv.at[g, a, 11 + tag], 0, d)
        if g == 0:
            for a in range(2):
                send_piece(g, a, 0)

    def step_b(g):
        b, n = GROUPS[g]
        h = n // 2
        for a in range(2):
            arrived(share_ref(a, 0, -1, b, h), g_recv.at[g, a, 0])
            send_group(a, share_ref(a, 0, -1, b, h), g_recv.at[g, a, 2], 0, 1)
            arrived(share_ref(a, 0, 1, b + h, h), g_recv.at[g, a, 1])
            send_group(a, share_ref(a, 0, 1, b + h, h), g_recv.at[g, a, 2], 0, -1)
        for a in range(2):
            arrived(share_ref(a, 0, -1, b + h, h), g_recv.at[g, a, 11])
            arrived(share_ref(a, 0, 1, b, h), g_recv.at[g, a, 12])
            for piece in (1, 2) if g == 0 else (0, 1, 2):
                send_piece(g, a, piece)

    def step_c(g):
        b, n = GROUPS[g]
        for a in range(2):
            arrived(share_ref(a, 0, 2, b, n), g_recv.at[g, a, 2])
            send_piece(g, a, 3)

    def step_d(g, *pieces):
        b, n = GROUPS[g]
        h = n // 2
        for piece in pieces:
            dm, tag = PIECES[piece], 3 + 2 * piece
            for a in range(2):
                arrived(share_ref(a, -1, dm, b, n), g_recv.at[g, a, tag])
                send_group(a, share_ref(a, -1, dm, b, h), e_recv.at[g], 1, 0)
                arrived(share_ref(a, 1, dm, b, n), g_recv.at[g, a, tag + 1])
                send_group(a, share_ref(a, 1, dm, b + h, h), e_recv.at[g], -1, 0)

    def step_e(g):
        b, n = GROUPS[g]
        arrived(full.at[:, 0:4, pl.ds(b, n)], e_recv.at[g])

    def rows_of(a, chunk, b0):
        return jnp.concatenate([full[a, chunk * 4 + i, b0 : b0 + 8].reshape(256, COLS) for i in range(4)], axis=1)

    def chunk_in(cg, chunk, begin):
        ks = pl.ds(pl.multiple_of(chunk * 1024, 1024), 1024)
        rows = rows_of(0, chunk, cg * 8)
        for acc, w in ((acc0, wg), (acc1, wu)):
            v = nt(rows, w[:, ks])
            acc[cg] = v if begin else acc[cg] + v

    def chunk_back(cg, chunk, begin):
        ks = pl.ds(pl.multiple_of(chunk * 1024, 1024), 1024)
        v = nt(rows_of(1, chunk, cg * 8), wd[:, ks])
        acc2[cg] = v if begin else acc2[cg] + v

    def chunks(cg, offset, begin):
        chunk_in(cg, lax.rem(y + offset, 4), begin)
        chunk_back(cg, lax.rem(x + offset, 4), begin)

    def activations(cg):
        gate, up, back = acc0[cg, :, :448], acc1[cg], acc2[cg, :, :448]
        s = jax.nn.sigmoid(gate)
        gated = gate * s
        hidden = (gated * up).astype(BF16)
        d_up = (back * gated).astype(BF16)
        d_gate = (back * up * s * (1.0 + gate * (1.0 - s))).astype(BF16)
        sums = nt(d_up, pbt1[...]) + nt(d_gate, pbt2[...]) + nt(hidden, pat[...])
        part[cg] = sums.astype(BF16).reshape(16, 16, 256)

    def scatter(cg):
        for dy, dx in PLANE:
            remote(
                part.at[cg, plane_index(dy, dx)],
                gathered.at[cg, me],
                rs_send.at[cg],
                rs_recv.at[cg],
                plane(dy, dx),
            )

    def gather(cg):
        total = part[cg, me].astype(F32)
        arrived(gathered.at[cg, 0:15], rs_recv.at[cg])
        for dy, dx in PLANE:
            total = total + gathered[cg, plane_index(dy, dx)].astype(F32)
        own[cg] = total.astype(BF16)
        for dy, dx in PLANE:
            remote(own.at[cg], factors.at[cg, me], ag_send.at[cg], ag_recv.at[cg], plane(dy, dx))
        factors[cg, me] = total.astype(BF16)

    low_half = iota((256, 128), 1) < 64
    pairs = iota((128, 256), 1) // 16 * 2

    def picked(shift, odd):
        return (iota((128, 256), 0) == pairs + (shift + odd)).astype(F32).astype(BF16)

    def spread(values, odd):
        high, low = split(values)
        return nn(high, picked(64, odd)) + nn(low, picked(64, odd))

    def against(values, w):
        high, low = split(values)
        return nt(high, w) + nt(low, w)

    def local_terms(cg):
        a_in, b_out = acc0[cg, :, 384:512], acc2[cg, :, 384:512]
        out_turned = pltpu.roll(b_out, 64, 1)
        terms[cg, 0] = spread(a_in, 0)
        terms[cg, 1] = spread(a_in, 1)
        terms[cg, 2] = against(jnp.where(low_half, out_turned, 0.0), wq0[...])
        terms[cg, 3] = against(jnp.where(low_half, 0.0, b_out), wq0[...])

    def scores(cg):
        arrived(factors.at[cg, 0:15], ag_recv.at[cg])
        all_rows = factors[cg].reshape(256, 256)
        b_both = all_rows[:, :128].astype(F32)
        b_turned = pltpu.roll(b_both, 64, 1)
        a_hidden = all_rows[:, 128:]
        even = jnp.concatenate([jnp.where(low_half, b_both, 0.0), jnp.where(low_half, b_turned, 0.0)], axis=1)
        odd = jnp.concatenate([jnp.where(low_half, 0.0, b_turned), jnp.where(low_half, 0.0, b_both)], axis=1)
        z_sum = terms[cg, 0] * nt(even.astype(BF16), wq12[...])
        z_sum += terms[cg, 1] * nt(odd.astype(BF16), wq12[...])
        z_sum += nn(a_hidden, picked(0, 0)) * terms[cg, 2]
        z_sum += nn(a_hidden, picked(0, 1)) * terms[cg, 3]
        high, low = split(z_sum)
        fold = (lax.rem(iota((16, 256), 1), 16) == iota((16, 256), 0)).astype(F32).astype(BF16)
        score = nt(fold, high) + nt(fold, low)
        for t in range(2):
            score_send[cg, t] = score[:, t * 128 : (t + 1) * 128]
        for pos in range(cg * 4, cg * 4 + 4):
            tile = score_send.at[cg, (pos % 4) // 2]
            for core in range(2):
                if pos != LOCAL:
                    remote(
                        tile,
                        score_recv.at[2 * pos + c],
                        sc_send,
                        sc_recv,
                        back_column(pos, core),
                    )
            if pos == LOCAL:
                remote(
                    tile,
                    score_recv.at[2 * pos + c],
                    sc_send,
                    sc_recv,
                    device(y, z * 2 + other, x),
                )
                score_recv[2 * pos + c] = score_send[cg, (pos % 4) // 2]
        share = jnp.zeros((16, 128), F32)
        for t in range(2):
            w_tile = jnp.zeros((1, 128), F32)
            for k in range(4):
                w_tile = w_tile + wrecv[cg * 8 + t * 4 + k]
            share = share + score[:, t * 128 : (t + 1) * 128] * w_tile
        return jnp.sum(share, axis=1, keepdims=True)

    def constants():
        wg[480:512] = jnp.zeros((32, 4096), BF16)
        loads["q"].wait()
        for i in range(16):
            wq0[i * 16 : (i + 1) * 16, :] = qs[:, i * 128 : (i + 1) * 128]
            wq12[i * 16 : (i + 1) * 16, 0:128] = qs[:, 2048 + i * 128 : 2048 + (i + 1) * 128]
            wq12[i * 16 : (i + 1) * 16, 128:256] = qs[:, 4096 + i * 128 : 4096 + (i + 1) * 128]
        loads["pa"].wait()
        loads["pb"].wait()
        at = iota((256, 64), 0) - iota((256, 64), 1)
        pbt1[...] = nn((at == 0).astype(F32).astype(BF16), pb[...]).astype(BF16)
        pbt2[...] = nn((at == 64).astype(F32).astype(BF16), pb[...]).astype(BF16)
        at = iota((256, 32), 0) - iota((256, 32), 1)
        pat[...] = nn((at == 128).astype(F32).astype(BF16), pa[...]).astype(BF16)

    def send_weights():
        for pos in range(NZ):
            if pos == LOCAL:
                remote(
                    wrow.at[2 * pos + other],
                    wrecv.at[2 * pos + c],
                    w_send,
                    w_recv,
                    device(y, z * 2 + other, x),
                )
                wrecv[2 * pos + c] = wrow[2 * pos + c]
            else:
                for core in range(2):
                    remote(
                        wrow.at[2 * pos + core],
                        wrecv.at[2 * pos + c],
                        w_send,
                        w_recv,
                        column(pos, core),
                    )

    chip_rows()
    slot_weights()
    constants()
    send_far(2, 3)
    step_a(0)
    send_far(4)
    send_pair()
    send_near()
    send_weights()
    step_b(0)
    step_a(1)
    step_c(0)
    step_d(0, 0)
    step_a(2)
    step_b(1)
    step_d(0, 1, 2)
    step_c(1)
    step_d(0, 3)
    step_b(2)
    for name in ("pin", "pout", "wg", "wu", "wd"):
        loads[name].wait()
    chunks(0, 0, True)
    step_d(1, 0)
    step_d(1, 1, 2)
    step_d(1, 3)
    chunks(0, 1, False)
    step_c(2)
    step_d(2, 0)
    chunks(0, 3, False)
    step_d(2, 1, 2)
    arrived(full.at[:, :, 2 * NEAR : 2 * NEAR + 4], near_recv)
    arrived(full.at[:, :, 2 * LOCAL + other], pair_recv)
    chunks(1, 0, True)
    step_d(2, 3)
    step_e(0)
    step_e(1)
    chunks(0, 2, False)
    activations(0)
    scatter(0)
    chunks(1, 1, False)
    chunks(1, 3, False)
    step_e(2)
    chunks(1, 2, False)
    activations(1)
    scatter(1)
    arrived(wrecv.at[0:15], w_recv)
    local_terms(0)
    gather(0)
    local_terms(1)
    gather(1)
    total0 = scores(0)
    total = total0 + scores(1)

    on_diagonal = iota((16, 128), 0) == iota((16, 128), 1)
    row = jnp.sum(jnp.where(on_diagonal, total, 0.0), axis=0, keepdims=True)
    tot_send[...] = row
    tot_recv[2 * LOCAL + c] = row
    for pos in FAR_FIRST:
        for core in range(2):
            if pos != LOCAL:
                remote(tot_send, tot_recv.at[2 * pos + c], t_send, t_recv, back_column(pos, core))
    remote(
        tot_send,
        tot_recv.at[2 * LOCAL + c],
        t_send,
        t_recv,
        device(y, z * 2 + other, x),
    )

    arrived(score_recv.at[0:15], sc_recv)
    every = jnp.concatenate([score_recv[k] for k in range(16)], axis=1)
    high, low = split(every)
    tok_ref[...] = nn(high, wm_hi[...]) + nn(high, wm_lo[...]) + nn(low, wm_hi[...])
    arrived(tot_recv.at[0:15], t_recv)
    row = tot_recv[0]
    for k in range(1, 16):
        row = row + tot_recv[k]
    tot_ref[...] = row[:, :16]
    left(full.at[:, 0:9, 0:10], z_send)
    left(full.at[:, 0:15, 0:10], g_send)
    left(wrecv.at[0:15], w_send)
    for cg in range(2):
        left(part.at[cg, 0:15], rs_send.at[cg])
        left(factors.at[cg, 0:15], ag_send.at[cg])
    left(score_recv.at[0:15], sc_send)
    left(tot_recv.at[0:15], t_send)


def results(scores_ref, totals_ref, scores_out, totals_out):
    scores_out[...] = scores_ref[...]
    totals_out[...] = totals_ref[...] * (1.0 / math.sqrt(2048.0))


def body(inputs, cotangents, routes, gates, w_gate, w_up, w_down, proj_in, proj_out, proj_hid_a, proj_hid_b, queries):
    anywhere = pl.BlockSpec(memory_space=pl.ANY)
    vmem = pl.BlockSpec(memory_space=pltpu.VMEM)
    scores, totals = pl.pallas_call(
        kernel,
        out_shape=(jax.ShapeDtypeStruct((16, 128), F32), jax.ShapeDtypeStruct((1, 16), F32)),
        in_specs=[anywhere] * 12,
        out_specs=(vmem, vmem),
        scratch_shapes=[
            pltpu.VMEM((128, 4096), BF16),
            pltpu.VMEM((128, 4096), BF16),
            pltpu.VMEM((2, 128), I32),
            pltpu.VMEM((2, 128), F32),
            pltpu.VMEM((512, 4096), BF16),
            pltpu.VMEM((448, 4096), BF16),
            pltpu.VMEM((512, 4096), BF16),
            pltpu.VMEM((32, 448), BF16),
            pltpu.VMEM((64, 448), BF16),
            pltpu.VMEM((16, 6144), BF16),
            pltpu.VMEM((2, SHARES, 16, SLOTS, COLS), BF16),
            pltpu.VMEM((2, 10, SLOTS, COLS), BF16),
            pltpu.VMEM((2, SHARES, SLOTS, COLS), BF16),
            pltpu.VMEM((2, 4, SHARES, SLOTS, COLS), BF16),
            pltpu.VMEM((2, 256, 512), F32),
            pltpu.VMEM((2, 256, 448), F32),
            pltpu.VMEM((2, 256, 512), F32),
            pltpu.VMEM((2, 4, 256, 256), F32),
            pltpu.VMEM((256, 448), BF16),
            pltpu.VMEM((256, 448), BF16),
            pltpu.VMEM((256, 448), BF16),
            pltpu.VMEM((256, 128), BF16),
            pltpu.VMEM((256, 256), BF16),
            pltpu.VMEM((2048, 128), BF16),
            pltpu.VMEM((2048, 128), BF16),
            pltpu.VMEM((16, 1, 128), F32),
            pltpu.VMEM((16, 1, 128), F32),
            pltpu.VMEM((2, 16, 16, 256), BF16),
            pltpu.VMEM((2, 16, 16, 256), BF16),
            pltpu.VMEM((2, 16, 256), BF16),
            pltpu.VMEM((2, 16, 16, 256), BF16),
            pltpu.VMEM((2, 2, 16, 128), F32),
            pltpu.VMEM((16, 16, 128), F32),
            pltpu.VMEM((1, 128), F32),
            pltpu.VMEM((16, 1, 128), F32),
            pltpu.SemaphoreType.DMA((12,)),
            pltpu.SemaphoreType.DMA,
            pltpu.SemaphoreType.DMA((3, 2)),
            pltpu.SemaphoreType.DMA,
            pltpu.SemaphoreType.DMA,
            pltpu.SemaphoreType.DMA,
            pltpu.SemaphoreType.DMA,
            pltpu.SemaphoreType.DMA,
            pltpu.SemaphoreType.DMA((3, 2, 13)),
            pltpu.SemaphoreType.DMA((3,)),
            pltpu.SemaphoreType.DMA((2,)),
            pltpu.SemaphoreType.DMA((2,)),
            pltpu.SemaphoreType.DMA((2,)),
            pltpu.SemaphoreType.DMA((2,)),
            pltpu.SemaphoreType.DMA,
            pltpu.SemaphoreType.DMA,
            pltpu.SemaphoreType.DMA,
            pltpu.SemaphoreType.DMA,
        ],
        compiler_params=pltpu.CompilerParams(
            collective_id=0, has_side_effects=True, vmem_limit_bytes=60 * 1024 * 1024
        ),
    )(
        inputs,
        cotangents,
        routes.T,
        gates.T,
        w_gate[0].T,
        w_up[0].T,
        w_down[0],
        proj_in.T,
        proj_out.T,
        proj_hid_a.T,
        proj_hid_b.T,
        queries,
    )
    scores, totals = pl.pallas_call(
        results,
        out_shape=(jax.ShapeDtypeStruct((16, 128), F32), jax.ShapeDtypeStruct((1, 16), F32)),
    )(scores, totals)
    return scores.T, totals.reshape(16)


def solution(mesh):
    placed = (
        P("expert", None),
        P("expert", None),
        P("expert", None),
        P("expert", None),
        P("expert", None, ("dp", "pipe")),
        P("expert", None, ("dp", "pipe")),
        P("expert", ("dp", "pipe"), None),
        P(),
        P(),
        P(("dp", "pipe"), None),
        P(("dp", "pipe"), None),
        P(("dp", "pipe"), None),
    )
    return jax.shard_map(
        body,
        mesh=mesh,
        in_specs=placed,
        out_specs=(P("expert", ("dp", "pipe")), P(("dp", "pipe"))),
        check_vma=False,
    )
```

```python
import math

import jax
import jax.numpy as jnp
from jax import lax
from jax.experimental import pallas as pl
from jax.experimental.pallas import tpu as pltpu
from jax.sharding import PartitionSpec as P

MESH = pl.DeviceIdType.MESH
F32, BF16, I32 = jnp.float32, jnp.bfloat16, jnp.int32

NZ = 8
ORDER = (2, 6, 3, 5, 4, 0, 1, 7)
LOCAL = ORDER.index(0)
FIRST = (0, 1, LOCAL, 6, 7)
NEAR = 6
SLOTS = 32
COLS = 256
SHARES = 16
GROUPS = ((0, 4), (4, 4), (8, 2))
PIECES = (0, -1, 1, 2)
PLANE = sorted(
    ((dy, dx) for dy in range(4) for dx in range(4) if dy or dx),
    key=lambda o: -min(o[0], 4 - o[0]) - min(o[1], 4 - o[1]),
)
FAR_FIRST = sorted(range(NZ), key=lambda i: -min(ORDER[i], NZ - ORDER[i]))


def nn(a, b):
    return lax.dot_general(a, b, (((1,), (0,)), ((), ())), preferred_element_type=F32)


def nt(a, b):
    return lax.dot_general(a, b, (((1,), (1,)), ((), ())), preferred_element_type=F32)


def iota(shape, dim):
    return lax.broadcasted_iota(I32, shape, dim)


def split(v):
    high = v.astype(BF16)
    return high, (v - high.astype(F32)).astype(BF16)


def kernel(
    x_hbm, g_hbm, routes_hbm, gates_hbm, wg_hbm, wu_hbm, wd_hbm, pin_hbm, pout_hbm, pa_hbm, pb_hbm, q_hbm,
    tok_ref, tot_ref,
    xs, gs, routes, gates, wg, wu, wd, pa, pb, qs,
    full, out_rows, out_pair, out_near, acc0, acc1, acc2, terms,
    pat, pbt1, pbt2, wq0, wq12, wm_hi, wm_lo, wrow, wrecv,
    part, gathered, own, factors, score_send, score_recv, tot_send, tot_recv,
    load_sem, z_send, z_recv, pair_recv, near_recv, w_send, w_recv,
    g_send, g_recv, e_recv, rs_send, rs_recv, ag_send, ag_recv, sc_send, sc_recv, t_send, t_recv,
    passed,
):
    y, e, x = lax.axis_index("dp"), lax.axis_index("expert"), lax.axis_index("pipe")
    z, c = lax.div(e, 2), lax.rem(e, 2)
    other = 1 - c
    me = y * 4 + x

    def device(yy, ee, xx):
        return {"dp": yy, "expert": ee, "pipe": xx}

    def column(pos, core):
        return device(y, lax.rem(z + ORDER[pos], NZ) * 2 + core, x)

    def back_column(pos, core):
        return device(y, lax.rem(z + NZ - ORDER[pos], NZ) * 2 + core, x)

    def plane(dy, dx):
        return device(lax.rem(y + dy, 4), e, lax.rem(x + dx, 4))

    def plane_index(dy, dx):
        return lax.rem(y + dy, 4) * 4 + lax.rem(x + dx, 4)

    def remote(src, dst, ss, rs, dev):
        pltpu.make_async_remote_copy(
            src_ref=src, dst_ref=dst, send_sem=ss, recv_sem=rs, device_id=dev, device_id_type=MESH
        ).start()

    def arrived(dst, rs):
        pltpu.make_async_remote_copy(
            src_ref=dst, dst_ref=dst, send_sem=rs, recv_sem=rs, device_id=device(y, e, x), device_id_type=MESH
        ).wait_recv()

    def left(src, ss):
        pltpu.make_async_remote_copy(
            src_ref=src, dst_ref=src, send_sem=ss, recv_sem=ss, device_id=device(y, e, x), device_id_type=MESH
        ).wait_send()

    barrier = pltpu.get_barrier_semaphore()
    for dy, dx in ((0, 1), (0, 3), (1, 0), (3, 0)):
        pl.semaphore_signal(barrier, inc=1, device_id=plane(dy, dx), device_id_type=MESH)
    for pos in FIRST:
        if pos == LOCAL:
            pl.semaphore_signal(barrier, inc=1, device_id=column(pos, other), device_id_type=MESH)
        else:
            for core in range(2):
                pl.semaphore_signal(barrier, inc=1, device_id=column(pos, core), device_id_type=MESH)

    loads = {}
    for i, (name, src, dst) in enumerate(
        (
            ("routes", routes_hbm, routes),
            ("gates", gates_hbm, gates),
            ("x", x_hbm, xs),
            ("g", g_hbm, gs),
            ("q", q_hbm, qs),
            ("pa", pa_hbm, pa),
            ("pb", pb_hbm, pb),
            ("pin", pin_hbm, wg.at[448:480]),
            ("pout", pout_hbm, wd.at[448:512]),
            ("wg", wg_hbm, wg.at[0:448]),
            ("wu", wu_hbm, wu),
            ("wd", wd_hbm, wd.at[0:448]),
        )
    ):
        loads[name] = pltpu.make_async_copy(src, dst, load_sem.at[i])
        loads[name].start()

    loads["routes"].wait()
    loads["gates"].wait()
    first, second = routes[0:1, :], routes[1:2, :]
    expert_rows = iota((16, 128), 0)
    named = ((expert_rows == first) | (expert_rows == second)).astype(F32)
    before = (iota((128, 128), 0) < iota((128, 128), 1)).astype(F32)
    earlier = nn(named.astype(BF16), before.astype(BF16))

    def places(route):
        slot = jnp.sum(jnp.where(expert_rows == route, earlier, 0.0), axis=0, keepdims=True).astype(I32)
        offset = ((route >> 1) - z) & (NZ - 1)
        pos = jnp.zeros_like(offset)
        for i, o in enumerate(ORDER):
            pos = jnp.where(offset == o, i, pos)
        block = pos * 2 + (route & 1)
        lane = block * 128 + ((pos & 1) * 2 + c) * 32 + slot
        return block * SLOTS + slot, lane

    place0, lane0 = places(first)
    place1, lane1 = places(second)

    def picks_of(start, count):
        rows = iota((count, 128), 0) + start
        return ((rows == place0) | (rows == place1)).astype(F32).astype(BF16)

    far = 10 * SLOTS
    picks = picks_of(0, far)
    shares = (y * 4 + x, x * 4 + y)
    for a, (name, source) in enumerate((("x", xs), ("g", gs))):
        loads[name].wait()
        columns = pl.ds(pl.multiple_of(shares[a] * COLS, COLS), COLS)
        rows = nn(picks, source[:, columns]).astype(BF16)
        out_rows[a] = rows.reshape(10, SLOTS, COLS)

    pl.semaphore_wait(barrier, 13)

    def send_far(*positions):
        for pos in positions:
            for a in range(2):
                for core in range(2):
                    remote(
                        out_rows.at[a, 2 * pos + core],
                        full.at[a, shares[a], 2 * pos + c],
                        z_send,
                        z_recv.at[pos // 2, a],
                        column(pos, core),
                    )

    send_far(0, 1)
    for pos in range(NEAR, NZ):
        for core in range(2):
            pl.semaphore_signal(passed, inc=1, device_id=column(pos, core), device_id_type=MESH)

    near_picks = picks_of(2 * NEAR * SLOTS, 4 * SLOTS)
    for a, source in enumerate((xs, gs)):
        for p in range(SHARES):
            rows = nn(near_picks, source[:, p * COLS : (p + 1) * COLS]).astype(BF16)
            out_near[a, :, p] = rows.reshape(4, SLOTS, COLS)

    def send_near():
        for a in range(2):
            for core in range(2):
                for pos in range(NEAR, NZ):
                    k = 2 * (pos - NEAR)
                    remote(
                        out_near.at[a, k + core],
                        full.at[a, :, 2 * pos + c],
                        z_send,
                        near_recv,
                        column(pos, core),
                    )

    def chip_rows():
        pair_picks = picks_of((2 * LOCAL + other) * SLOTS, SLOTS)
        own_picks = picks_of((2 * LOCAL + c) * SLOTS, SLOTS)
        for a, source in enumerate((xs, gs)):
            for p in range(SHARES):
                columns = source[:, p * COLS : (p + 1) * COLS]
                out_pair[a, p] = nn(pair_picks, columns).astype(BF16)
                full[a, p, 2 * LOCAL + c] = nn(own_picks, columns).astype(BF16)

    def send_pair():
        for a in range(2):
            remote(
                out_pair.at[a],
                full.at[a, :, 2 * LOCAL + c],
                z_send,
                pair_recv,
                device(y, z * 2 + other, x),
            )

    def slot_weights():
        lanes = iota((2048, 128), 0)
        weights = jnp.where(lanes == lane0, gates[0:1, :], 0.0) + jnp.where(lanes == lane1, gates[1:2, :], 0.0)
        high, low = split(weights)
        wm_hi[...] = high
        wm_lo[...] = low
        ones = jnp.ones((8, 128), BF16)
        sums = nt(ones, high) + nt(ones, low)
        for k in range(16):
            wrow[k] = sums[0:1, k * 128 : (k + 1) * 128]

    def ring(a, major, minor):
        major, minor = lax.rem(major + 4, 4), lax.rem(minor + 4, 4)
        return device(major, e, minor) if a == 0 else device(minor, e, major)

    mine = ((y, x), (x, y))

    def share_ref(a, dmajor, dminor, first_block, blocks):
        major, minor = mine[a]
        share = lax.rem(major + dmajor + 4, 4) * 4 + lax.rem(minor + dminor + 4, 4)
        return full.at[a, share, pl.ds(first_block, blocks)]

    def send_group(a, ref, sem, dmajor, dminor):
        major, minor = mine[a]
        remote(ref, ref, g_send, sem, ring(a, major + dmajor, minor + dminor))

    def send_piece(g, a, piece):
        b, n = GROUPS[g]
        for way, d in enumerate((1, -1)):
            send_group(a, share_ref(a, 0, PIECES[piece], b, n), g_recv.at[g, a, 3 + 2 * piece + way], d, 0)

    def step_a(g):
        b, n = GROUPS[g]
        h = n // 2
        for a in range(2):
            arrived(share_ref(a, 0, 0, b, n), z_recv.at[g, a])
            for tag, first in ((0, b), (1, b + h)):
                other_half = b + h if tag == 0 else b
                d = 1 if tag == 0 else -1
                send_group(a, share_ref(a, 0, 0, first, h), g_recv.at[g, a, tag], 0, d)
                send_group(a, share_ref(a, 0, 0, other_half, h), g_recv.at[g, a, 11 + tag], 0, d)
        if g == 0:
            for a in range(2):
                send_piece(g, a, 0)

    def step_b(g):
        b, n = GROUPS[g]
        h = n // 2
        for a in range(2):
            arrived(share_ref(a, 0, -1, b, h), g_recv.at[g, a, 0])
            send_group(a, share_ref(a, 0, -1, b, h), g_recv.at[g, a, 2], 0, 1)
            arrived(share_ref(a, 0, 1, b + h, h), g_recv.at[g, a, 1])
            send_group(a, share_ref(a, 0, 1, b + h, h), g_recv.at[g, a, 2], 0, -1)
        for a in range(2):
            arrived(share_ref(a, 0, -1, b + h, h), g_recv.at[g, a, 11])
            arrived(share_ref(a, 0, 1, b, h), g_recv.at[g, a, 12])
            for piece in (1, 2) if g == 0 else (0, 1, 2):
                send_piece(g, a, piece)

    def step_c(g):
        b, n = GROUPS[g]
        for a in range(2):
            arrived(share_ref(a, 0, 2, b, n), g_recv.at[g, a, 2])
            send_piece(g, a, 3)

    def step_d(g, *pieces):
        b, n = GROUPS[g]
        h = n // 2
        for piece in pieces:
            dm, tag = PIECES[piece], 3 + 2 * piece
            for a in range(2):
                arrived(share_ref(a, -1, dm, b, n), g_recv.at[g, a, tag])
                send_group(a, share_ref(a, -1, dm, b, h), e_recv.at[g], 1, 0)
                arrived(share_ref(a, 1, dm, b, n), g_recv.at[g, a, tag + 1])
                send_group(a, share_ref(a, 1, dm, b + h, h), e_recv.at[g], -1, 0)

    def step_e(g):
        b, n = GROUPS[g]
        arrived(full.at[:, 0:4, pl.ds(b, n)], e_recv.at[g])

    def rows_of(a, chunk, b0):
        return jnp.concatenate([full[a, chunk * 4 + i, b0 : b0 + 8].reshape(256, COLS) for i in range(4)], axis=1)

    def chunk_in(cg, chunk, begin):
        ks = pl.ds(pl.multiple_of(chunk * 1024, 1024), 1024)
        rows = rows_of(0, chunk, cg * 8)
        for acc, w in ((acc0, wg), (acc1, wu)):
            v = nt(rows, w[:, ks])
            acc[cg] = v if begin else acc[cg] + v

    def chunk_back(cg, chunk, begin):
        ks = pl.ds(pl.multiple_of(chunk * 1024, 1024), 1024)
        v = nt(rows_of(1, chunk, cg * 8), wd[:, ks])
        acc2[cg] = v if begin else acc2[cg] + v

    def chunks(cg, offset, begin):
        chunk_in(cg, lax.rem(y + offset, 4), begin)
        chunk_back(cg, lax.rem(x + offset, 4), begin)

    def activations(cg):
        gate, up, back = acc0[cg, :, :448], acc1[cg], acc2[cg, :, :448]
        s = jax.nn.sigmoid(gate)
        gated = gate * s
        hidden = (gated * up).astype(BF16)
        d_up = (back * gated).astype(BF16)
        d_gate = (back * up * s * (1.0 + gate * (1.0 - s))).astype(BF16)
        sums = nt(d_up, pbt1[...]) + nt(d_gate, pbt2[...]) + nt(hidden, pat[...])
        part[cg] = sums.astype(BF16).reshape(16, 16, 256)

    def scatter(cg):
        for dy, dx in PLANE:
            remote(
                part.at[cg, plane_index(dy, dx)],
                gathered.at[cg, me],
                rs_send.at[cg],
                rs_recv.at[cg],
                plane(dy, dx),
            )

    def gather(cg):
        total = part[cg, me].astype(F32)
        arrived(gathered.at[cg, 0:15], rs_recv.at[cg])
        for dy, dx in PLANE:
            total = total + gathered[cg, plane_index(dy, dx)].astype(F32)
        own[cg] = total.astype(BF16)
        for dy, dx in PLANE:
            remote(own.at[cg], factors.at[cg, me], ag_send.at[cg], ag_recv.at[cg], plane(dy, dx))
        factors[cg, me] = total.astype(BF16)

    low_half = iota((256, 128), 1) < 64
    pairs = iota((128, 256), 1) // 16 * 2

    def picked(shift, odd):
        return (iota((128, 256), 0) == pairs + (shift + odd)).astype(F32).astype(BF16)

    def spread(values, odd):
        high, low = split(values)
        return nn(high, picked(64, odd)) + nn(low, picked(64, odd))

    def against(values, w):
        high, low = split(values)
        return nt(high, w) + nt(low, w)

    def local_terms(cg):
        a_in, b_out = acc0[cg, :, 384:512], acc2[cg, :, 384:512]
        out_turned = pltpu.roll(b_out, 64, 1)
        terms[cg, 0] = spread(a_in, 0)
        terms[cg, 1] = spread(a_in, 1)
        terms[cg, 2] = against(jnp.where(low_half, out_turned, 0.0), wq0[...])
        terms[cg, 3] = against(jnp.where(low_half, 0.0, b_out), wq0[...])

    def scores(cg):
        arrived(factors.at[cg, 0:15], ag_recv.at[cg])
        all_rows = factors[cg].reshape(256, 256)
        b_both = all_rows[:, :128].astype(F32)
        b_turned = pltpu.roll(b_both, 64, 1)
        a_hidden = all_rows[:, 128:]
        even = jnp.concatenate([jnp.where(low_half, b_both, 0.0), jnp.where(low_half, b_turned, 0.0)], axis=1)
        odd = jnp.concatenate([jnp.where(low_half, 0.0, b_turned), jnp.where(low_half, 0.0, b_both)], axis=1)
        z_sum = terms[cg, 0] * nt(even.astype(BF16), wq12[...])
        z_sum += terms[cg, 1] * nt(odd.astype(BF16), wq12[...])
        z_sum += nn(a_hidden, picked(0, 0)) * terms[cg, 2]
        z_sum += nn(a_hidden, picked(0, 1)) * terms[cg, 3]
        high, low = split(z_sum)
        fold = (lax.rem(iota((16, 256), 1), 16) == iota((16, 256), 0)).astype(F32).astype(BF16)
        score = nt(fold, high) + nt(fold, low)
        for t in range(2):
            score_send[cg, t] = score[:, t * 128 : (t + 1) * 128]
        for pos in range(cg * 4, cg * 4 + 4):
            tile = score_send.at[cg, (pos % 4) // 2]
            for core in range(2):
                if pos != LOCAL:
                    remote(
                        tile,
                        score_recv.at[2 * pos + c],
                        sc_send,
                        sc_recv,
                        back_column(pos, core),
                    )
            if pos == LOCAL:
                remote(
                    tile,
                    score_recv.at[2 * pos + c],
                    sc_send,
                    sc_recv,
                    device(y, z * 2 + other, x),
                )
                score_recv[2 * pos + c] = score_send[cg, (pos % 4) // 2]
        share = jnp.zeros((16, 128), F32)
        for t in range(2):
            w_tile = jnp.zeros((1, 128), F32)
            for k in range(4):
                w_tile = w_tile + wrecv[cg * 8 + t * 4 + k]
            share = share + score[:, t * 128 : (t + 1) * 128] * w_tile
        return jnp.sum(share, axis=1, keepdims=True)

    def constants():
        wg[480:512] = jnp.zeros((32, 4096), BF16)
        loads["q"].wait()
        for i in range(16):
            wq0[i * 16 : (i + 1) * 16, :] = qs[:, i * 128 : (i + 1) * 128]
            wq12[i * 16 : (i + 1) * 16, 0:128] = qs[:, 2048 + i * 128 : 2048 + (i + 1) * 128]
            wq12[i * 16 : (i + 1) * 16, 128:256] = qs[:, 4096 + i * 128 : 4096 + (i + 1) * 128]
        loads["pa"].wait()
        loads["pb"].wait()
        at = iota((256, 64), 0) - iota((256, 64), 1)
        pbt1[...] = nn((at == 0).astype(F32).astype(BF16), pb[...]).astype(BF16)
        pbt2[...] = nn((at == 64).astype(F32).astype(BF16), pb[...]).astype(BF16)
        at = iota((256, 32), 0) - iota((256, 32), 1)
        pat[...] = nn((at == 128).astype(F32).astype(BF16), pa[...]).astype(BF16)

    def send_weights():
        for pos in range(NZ):
            if pos == LOCAL:
                remote(
                    wrow.at[2 * pos + other],
                    wrecv.at[2 * pos + c],
                    w_send,
                    w_recv,
                    device(y, z * 2 + other, x),
                )
                wrecv[2 * pos + c] = wrow[2 * pos + c]
            else:
                for core in range(2):
                    remote(
                        wrow.at[2 * pos + core],
                        wrecv.at[2 * pos + c],
                        w_send,
                        w_recv,
                        column(pos, core),
                    )

    chip_rows()
    slot_weights()
    constants()
    pl.semaphore_wait(passed, 4)
    send_far(2, 3)
    step_a(0)
    send_far(4)
    send_pair()
    send_near()
    send_weights()
    step_b(0)
    step_a(1)
    step_c(0)
    step_d(0, 0)
    step_a(2)
    step_b(1)
    step_d(0, 1, 2)
    step_b(2)
    step_c(1)
    step_d(0, 3)
    for name in ("pin", "pout", "wg", "wu", "wd"):
        loads[name].wait()
    chunks(0, 0, True)
    step_d(1, 0)
    step_d(1, 1, 2)
    step_c(2)
    step_d(2, 0)
    step_d(2, 1, 2)
    step_d(1, 3)
    chunks(0, 1, False)
    chunks(0, 3, False)
    arrived(full.at[:, :, 2 * NEAR : 2 * NEAR + 4], near_recv)
    arrived(full.at[:, :, 2 * LOCAL + other], pair_recv)
    chunks(1, 0, True)
    step_d(2, 3)
    chunks(1, 1, False)
    chunks(1, 3, False)
    step_e(0)
    step_e(1)
    chunks(0, 2, False)
    activations(0)
    scatter(0)
    step_e(2)
    chunks(1, 2, False)
    activations(1)
    scatter(1)
    arrived(wrecv.at[0:15], w_recv)
    local_terms(0)
    gather(0)
    local_terms(1)
    gather(1)
    total0 = scores(0)
    total = total0 + scores(1)

    on_diagonal = iota((16, 128), 0) == iota((16, 128), 1)
    row = jnp.sum(jnp.where(on_diagonal, total, 0.0), axis=0, keepdims=True)
    tot_send[...] = row
    tot_recv[2 * LOCAL + c] = row
    for pos in FAR_FIRST:
        for core in range(2):
            if pos != LOCAL:
                remote(tot_send, tot_recv.at[2 * pos + c], t_send, t_recv, back_column(pos, core))
    remote(
        tot_send,
        tot_recv.at[2 * LOCAL + c],
        t_send,
        t_recv,
        device(y, z * 2 + other, x),
    )

    arrived(score_recv.at[0:15], sc_recv)
    every = jnp.concatenate([score_recv[k] for k in range(16)], axis=1)
    high, low = split(every)
    tok_ref[...] = nn(high, wm_hi[...]) + nn(high, wm_lo[...]) + nn(low, wm_hi[...])
    arrived(tot_recv.at[0:15], t_recv)
    row = tot_recv[0]
    for k in range(1, 16):
        row = row + tot_recv[k]
    tot_ref[...] = row[:, :16]
    left(full.at[:, 0:9, 0:10], z_send)
    left(full.at[:, 0:15, 0:10], g_send)
    left(wrecv.at[0:15], w_send)
    for cg in range(2):
        left(part.at[cg, 0:15], rs_send.at[cg])
        left(factors.at[cg, 0:15], ag_send.at[cg])
    left(score_recv.at[0:15], sc_send)
    left(tot_recv.at[0:15], t_send)


def results(scores_ref, totals_ref, scores_out, totals_out):
    scores_out[...] = scores_ref[...]
    totals_out[...] = totals_ref[...] * (1.0 / math.sqrt(2048.0))


def body(inputs, cotangents, routes, gates, w_gate, w_up, w_down, proj_in, proj_out, proj_hid_a, proj_hid_b, queries):
    anywhere = pl.BlockSpec(memory_space=pl.ANY)
    vmem = pl.BlockSpec(memory_space=pltpu.VMEM)
    scores, totals = pl.pallas_call(
        kernel,
        out_shape=(jax.ShapeDtypeStruct((16, 128), F32), jax.ShapeDtypeStruct((1, 16), F32)),
        in_specs=[anywhere] * 12,
        out_specs=(vmem, vmem),
        scratch_shapes=[
            pltpu.VMEM((128, 4096), BF16),
            pltpu.VMEM((128, 4096), BF16),
            pltpu.VMEM((2, 128), I32),
            pltpu.VMEM((2, 128), F32),
            pltpu.VMEM((512, 4096), BF16),
            pltpu.VMEM((448, 4096), BF16),
            pltpu.VMEM((512, 4096), BF16),
            pltpu.VMEM((32, 448), BF16),
            pltpu.VMEM((64, 448), BF16),
            pltpu.VMEM((16, 6144), BF16),
            pltpu.VMEM((2, SHARES, 16, SLOTS, COLS), BF16),
            pltpu.VMEM((2, 10, SLOTS, COLS), BF16),
            pltpu.VMEM((2, SHARES, SLOTS, COLS), BF16),
            pltpu.VMEM((2, 4, SHARES, SLOTS, COLS), BF16),
            pltpu.VMEM((2, 256, 512), F32),
            pltpu.VMEM((2, 256, 448), F32),
            pltpu.VMEM((2, 256, 512), F32),
            pltpu.VMEM((2, 4, 256, 256), F32),
            pltpu.VMEM((256, 448), BF16),
            pltpu.VMEM((256, 448), BF16),
            pltpu.VMEM((256, 448), BF16),
            pltpu.VMEM((256, 128), BF16),
            pltpu.VMEM((256, 256), BF16),
            pltpu.VMEM((2048, 128), BF16),
            pltpu.VMEM((2048, 128), BF16),
            pltpu.VMEM((16, 1, 128), F32),
            pltpu.VMEM((16, 1, 128), F32),
            pltpu.VMEM((2, 16, 16, 256), BF16),
            pltpu.VMEM((2, 16, 16, 256), BF16),
            pltpu.VMEM((2, 16, 256), BF16),
            pltpu.VMEM((2, 16, 16, 256), BF16),
            pltpu.VMEM((2, 2, 16, 128), F32),
            pltpu.VMEM((16, 16, 128), F32),
            pltpu.VMEM((1, 128), F32),
            pltpu.VMEM((16, 1, 128), F32),
            pltpu.SemaphoreType.DMA((12,)),
            pltpu.SemaphoreType.DMA,
            pltpu.SemaphoreType.DMA((3, 2)),
            pltpu.SemaphoreType.DMA,
            pltpu.SemaphoreType.DMA,
            pltpu.SemaphoreType.DMA,
            pltpu.SemaphoreType.DMA,
            pltpu.SemaphoreType.DMA,
            pltpu.SemaphoreType.DMA((3, 2, 13)),
            pltpu.SemaphoreType.DMA((3,)),
            pltpu.SemaphoreType.DMA((2,)),
            pltpu.SemaphoreType.DMA((2,)),
            pltpu.SemaphoreType.DMA((2,)),
            pltpu.SemaphoreType.DMA((2,)),
            pltpu.SemaphoreType.DMA,
            pltpu.SemaphoreType.DMA,
            pltpu.SemaphoreType.DMA,
            pltpu.SemaphoreType.DMA,
            pltpu.SemaphoreType.REGULAR,
        ],
        compiler_params=pltpu.CompilerParams(
            collective_id=0, has_side_effects=True, vmem_limit_bytes=60 * 1024 * 1024
        ),
    )(
        inputs,
        cotangents,
        routes.T,
        gates.T,
        w_gate[0].T,
        w_up[0].T,
        w_down[0],
        proj_in.T,
        proj_out.T,
        proj_hid_a.T,
        proj_hid_b.T,
        queries,
    )
    scores, totals = pl.pallas_call(
        results,
        out_shape=(jax.ShapeDtypeStruct((16, 128), F32), jax.ShapeDtypeStruct((1, 16), F32)),
    )(scores, totals)
    return scores.T, totals.reshape(16)


def solution(mesh):
    placed = (
        P("expert", None),
        P("expert", None),
        P("expert", None),
        P("expert", None),
        P("expert", None, ("dp", "pipe")),
        P("expert", None, ("dp", "pipe")),
        P("expert", ("dp", "pipe"), None),
        P(),
        P(),
        P(("dp", "pipe"), None),
        P(("dp", "pipe"), None),
        P(("dp", "pipe"), None),
    )
    return jax.shard_map(
        body,
        mesh=mesh,
        in_specs=placed,
        out_specs=(P("expert", ("dp", "pipe")), P(("dp", "pipe"))),
        check_vma=False,
    )
```

```python
import math

import jax
import jax.numpy as jnp
from jax import lax
from jax.experimental import pallas as pl
from jax.experimental.pallas import tpu as pltpu
from jax.sharding import PartitionSpec as P

MESH = pl.DeviceIdType.MESH
F32, BF16, I32 = jnp.float32, jnp.bfloat16, jnp.int32

NZ = 8
ORDER = (2, 6, 3, 5, 4, 0, 1, 7)
LOCAL = ORDER.index(0)
FIRST = (0, 1, LOCAL, 6, 7)
NEAR = 6
SLOTS = 32
COLS = 256
SHARES = 16
GROUPS = ((0, 4), (4, 4), (8, 2))
PIECES = (0, -1, 1, 2)
PLANE = sorted(
    ((dy, dx) for dy in range(4) for dx in range(4) if dy or dx),
    key=lambda o: -min(o[0], 4 - o[0]) - min(o[1], 4 - o[1]),
)
FAR_FIRST = sorted(range(NZ), key=lambda i: -min(ORDER[i], NZ - ORDER[i]))


def nn(a, b):
    return lax.dot_general(a, b, (((1,), (0,)), ((), ())), preferred_element_type=F32)


def nt(a, b):
    return lax.dot_general(a, b, (((1,), (1,)), ((), ())), preferred_element_type=F32)


def iota(shape, dim):
    return lax.broadcasted_iota(I32, shape, dim)


def split(v):
    high = v.astype(BF16)
    return high, (v - high.astype(F32)).astype(BF16)


def kernel(
    x_hbm, g_hbm, routes_hbm, gates_hbm, wg_hbm, wu_hbm, wd_hbm, pin_hbm, pout_hbm, pa_hbm, pb_hbm, q_hbm,
    tok_ref, tot_ref,
    xs, gs, routes, gates, wg, wu, wd, pa, pb, qs,
    full, out_rows, out_pair, out_near, acc0, acc1, acc2, terms,
    pat0, pat1, pbt1, pbt2, wq0, wq12, wm_hi, wm_lo, wrow, wrecv,
    part, gathered, own, factors, score_send, score_recv, tot_send, tot_recv,
    load_sem, z_send, z_recv, pair_recv, near_recv, w_send, w_recv,
    g_send, g_recv, e_recv, rs_send, rs_recv, ag_send, ag_recv, sc_send, sc_recv, t_send, t_recv,
    passed,
):
    y, e, x = lax.axis_index("dp"), lax.axis_index("expert"), lax.axis_index("pipe")
    z, c = lax.div(e, 2), lax.rem(e, 2)
    other = 1 - c
    me = y * 4 + x

    def device(yy, ee, xx):
        return {"dp": yy, "expert": ee, "pipe": xx}

    def column(pos, core):
        return device(y, lax.rem(z + ORDER[pos], NZ) * 2 + core, x)

    def back_column(pos, core):
        return device(y, lax.rem(z + NZ - ORDER[pos], NZ) * 2 + core, x)

    def plane(dy, dx):
        return device(lax.rem(y + dy, 4), e, lax.rem(x + dx, 4))

    def plane_index(dy, dx):
        return lax.rem(y + dy, 4) * 4 + lax.rem(x + dx, 4)

    def remote(src, dst, ss, rs, dev):
        pltpu.make_async_remote_copy(
            src_ref=src, dst_ref=dst, send_sem=ss, recv_sem=rs, device_id=dev, device_id_type=MESH
        ).start()

    def arrived(dst, rs):
        pltpu.make_async_remote_copy(
            src_ref=dst, dst_ref=dst, send_sem=rs, recv_sem=rs, device_id=device(y, e, x), device_id_type=MESH
        ).wait_recv()

    def left(src, ss):
        pltpu.make_async_remote_copy(
            src_ref=src, dst_ref=src, send_sem=ss, recv_sem=ss, device_id=device(y, e, x), device_id_type=MESH
        ).wait_send()

    barrier = pltpu.get_barrier_semaphore()
    for dy, dx in ((0, 1), (0, 3), (1, 0), (3, 0)):
        pl.semaphore_signal(barrier, inc=1, device_id=plane(dy, dx), device_id_type=MESH)
    for pos in FIRST:
        if pos == LOCAL:
            pl.semaphore_signal(barrier, inc=1, device_id=column(pos, other), device_id_type=MESH)
        else:
            for core in range(2):
                pl.semaphore_signal(barrier, inc=1, device_id=column(pos, core), device_id_type=MESH)

    loads = {}
    for i, (name, src, dst) in enumerate(
        (
            ("routes", routes_hbm, routes),
            ("gates", gates_hbm, gates),
            ("x", x_hbm, xs),
            ("g", g_hbm, gs),
            ("q", q_hbm, qs),
            ("pa", pa_hbm, pa),
            ("pb", pb_hbm, pb),
            ("pin", pin_hbm, wg.at[448:480]),
            ("pout", pout_hbm, wd.at[448:512]),
            ("wg", wg_hbm, wg.at[0:448]),
            ("wu", wu_hbm, wu),
            ("wd", wd_hbm, wd.at[0:448]),
        )
    ):
        loads[name] = pltpu.make_async_copy(src, dst, load_sem.at[i])
        loads[name].start()

    loads["routes"].wait()
    loads["gates"].wait()
    first, second = routes[0:1, :], routes[1:2, :]
    expert_rows = iota((16, 128), 0)
    named = ((expert_rows == first) | (expert_rows == second)).astype(F32)
    before = (iota((128, 128), 0) < iota((128, 128), 1)).astype(F32)
    earlier = nn(named.astype(BF16), before.astype(BF16))

    def places(route):
        slot = jnp.sum(jnp.where(expert_rows == route, earlier, 0.0), axis=0, keepdims=True).astype(I32)
        offset = ((route >> 1) - z) & (NZ - 1)
        pos = jnp.zeros_like(offset)
        for i, o in enumerate(ORDER):
            pos = jnp.where(offset == o, i, pos)
        block = pos * 2 + (route & 1)
        lane = block * 128 + ((pos & 1) * 2 + c) * 32 + slot
        return block * SLOTS + slot, lane

    place0, lane0 = places(first)
    place1, lane1 = places(second)

    def picks_of(start, count):
        rows = iota((count, 128), 0) + start
        return ((rows == place0) | (rows == place1)).astype(F32).astype(BF16)

    far = 10 * SLOTS
    picks = picks_of(0, far)
    shares = (y * 4 + x, x * 4 + y)
    for a, (name, source) in enumerate((("x", xs), ("g", gs))):
        loads[name].wait()
        columns = pl.ds(pl.multiple_of(shares[a] * COLS, COLS), COLS)
        rows = nn(picks, source[:, columns]).astype(BF16)
        out_rows[a] = rows.reshape(10, SLOTS, COLS)

    pl.semaphore_wait(barrier, 13)

    def send_far(*positions):
        for pos in positions:
            for a in range(2):
                for core in range(2):
                    remote(
                        out_rows.at[a, 2 * pos + core],
                        full.at[a, shares[a], 2 * pos + c],
                        z_send,
                        z_recv.at[pos // 2, a],
                        column(pos, core),
                    )

    send_far(0, 1)
    for pos in range(NEAR, NZ):
        for core in range(2):
            pl.semaphore_signal(passed, inc=1, device_id=column(pos, core), device_id_type=MESH)

    near_picks = picks_of(2 * NEAR * SLOTS, 4 * SLOTS)
    for a, source in enumerate((xs, gs)):
        for p in range(SHARES):
            rows = nn(near_picks, source[:, p * COLS : (p + 1) * COLS]).astype(BF16)
            out_near[a, :, p] = rows.reshape(4, SLOTS, COLS)

    def send_near():
        for a in range(2):
            for core in range(2):
                for pos in range(NEAR, NZ):
                    k = 2 * (pos - NEAR)
                    remote(
                        out_near.at[a, k + core],
                        full.at[a, :, 2 * pos + c],
                        z_send,
                        near_recv,
                        column(pos, core),
                    )

    def chip_rows():
        pair_picks = picks_of((2 * LOCAL + other) * SLOTS, SLOTS)
        own_picks = picks_of((2 * LOCAL + c) * SLOTS, SLOTS)
        for a, source in enumerate((xs, gs)):
            for p in range(SHARES):
                columns = source[:, p * COLS : (p + 1) * COLS]
                out_pair[a, p] = nn(pair_picks, columns).astype(BF16)
                full[a, p, 2 * LOCAL + c] = nn(own_picks, columns).astype(BF16)

    def send_pair():
        for a in range(2):
            remote(
                out_pair.at[a],
                full.at[a, :, 2 * LOCAL + c],
                z_send,
                pair_recv,
                device(y, z * 2 + other, x),
            )

    def slot_weights():
        lanes = iota((2048, 128), 0)
        weights = jnp.where(lanes == lane0, gates[0:1, :], 0.0) + jnp.where(lanes == lane1, gates[1:2, :], 0.0)
        high, low = split(weights)
        wm_hi[...] = high
        wm_lo[...] = low
        ones = jnp.ones((8, 128), BF16)
        sums = nt(ones, high) + nt(ones, low)
        for k in range(16):
            wrow[k] = sums[0:1, k * 128 : (k + 1) * 128]

    def ring(a, major, minor):
        major, minor = lax.rem(major + 4, 4), lax.rem(minor + 4, 4)
        return device(major, e, minor) if a == 0 else device(minor, e, major)

    mine = ((y, x), (x, y))

    def share_ref(a, dmajor, dminor, first_block, blocks):
        major, minor = mine[a]
        share = lax.rem(major + dmajor + 4, 4) * 4 + lax.rem(minor + dminor + 4, 4)
        return full.at[a, share, pl.ds(first_block, blocks)]

    def send_group(a, ref, sem, dmajor, dminor):
        major, minor = mine[a]
        remote(ref, ref, g_send, sem, ring(a, major + dmajor, minor + dminor))

    def send_piece(g, a, piece):
        b, n = GROUPS[g]
        for way, d in enumerate((1, -1)):
            send_group(a, share_ref(a, 0, PIECES[piece], b, n), g_recv.at[g, a, 3 + 2 * piece + way], d, 0)

    def step_a(g):
        b, n = GROUPS[g]
        h = n // 2
        for a in range(2):
            arrived(share_ref(a, 0, 0, b, n), z_recv.at[g, a])
            for tag, first in ((0, b), (1, b + h)):
                other_half = b + h if tag == 0 else b
                d = 1 if tag == 0 else -1
                send_group(a, share_ref(a, 0, 0, first, h), g_recv.at[g, a, tag], 0, d)
                send_group(a, share_ref(a, 0, 0, other_half, h), g_recv.at[g, a, 11 + tag], 0, d)
        if g == 0:
            for a in range(2):
                send_piece(g, a, 0)

    def step_b(g):
        b, n = GROUPS[g]
        h = n // 2
        for a in range(2):
            arrived(share_ref(a, 0, -1, b, h), g_recv.at[g, a, 0])
            send_group(a, share_ref(a, 0, -1, b, h), g_recv.at[g, a, 2], 0, 1)
            arrived(share_ref(a, 0, 1, b + h, h), g_recv.at[g, a, 1])
            send_group(a, share_ref(a, 0, 1, b + h, h), g_recv.at[g, a, 2], 0, -1)
        for a in range(2):
            arrived(share_ref(a, 0, -1, b + h, h), g_recv.at[g, a, 11])
            arrived(share_ref(a, 0, 1, b, h), g_recv.at[g, a, 12])
            for piece in (1, 2) if g == 0 else (0, 1, 2):
                send_piece(g, a, piece)

    def step_c(g):
        b, n = GROUPS[g]
        for a in range(2):
            arrived(share_ref(a, 0, 2, b, n), g_recv.at[g, a, 2])
            send_piece(g, a, 3)

    def step_d(g, *pieces):
        b, n = GROUPS[g]
        h = n // 2
        for piece in pieces:
            dm, tag = PIECES[piece], 3 + 2 * piece
            for a in range(2):
                arrived(share_ref(a, -1, dm, b, n), g_recv.at[g, a, tag])
                send_group(a, share_ref(a, -1, dm, b, h), e_recv.at[g], 1, 0)
                arrived(share_ref(a, 1, dm, b, n), g_recv.at[g, a, tag + 1])
                send_group(a, share_ref(a, 1, dm, b + h, h), e_recv.at[g], -1, 0)

    def step_e(g):
        b, n = GROUPS[g]
        arrived(full.at[:, 0:4, pl.ds(b, n)], e_recv.at[g])

    def rows_of(a, chunk, b0):
        return jnp.concatenate([full[a, chunk * 4 + i, b0 : b0 + 8].reshape(256, COLS) for i in range(4)], axis=1)

    def chunk_in(cg, chunk, begin):
        ks = pl.ds(pl.multiple_of(chunk * 1024, 1024), 1024)
        rows = rows_of(0, chunk, cg * 8)
        for acc, w in ((acc0, wg), (acc1, wu)):
            v = nt(rows, w[:, ks])
            acc[cg] = v if begin else acc[cg] + v

    def chunk_back(cg, chunk, begin):
        ks = pl.ds(pl.multiple_of(chunk * 1024, 1024), 1024)
        v = nt(rows_of(1, chunk, cg * 8), wd[:, ks])
        acc2[cg] = v if begin else acc2[cg] + v

    def chunks(cg, offset, begin):
        chunk_in(cg, lax.rem(y + offset, 4), begin)
        chunk_back(cg, lax.rem(x + offset, 4), begin)

    def activations(cg):
        gate, up, back = acc0[cg, :, :448], acc1[cg], acc2[cg, :, :448]
        s = jax.nn.sigmoid(gate)
        gated = gate * s
        hidden = (gated * up).astype(BF16)
        d_up = (back * gated).astype(BF16)
        d_gate = (back * up * s * (1.0 + gate * (1.0 - s))).astype(BF16)
        grads = nt(d_up, pbt1[...]) + nt(d_gate, pbt2[...])
        halves = nt(hidden[0:128], pat0[...]) + nt(hidden[128:256], pat1[...])
        part[cg, :, 0:16] = grads.reshape(16, 16, 128).astype(BF16)
        part[cg, :, 16:24] = halves.reshape(16, 8, 128).astype(BF16)

    def scatter(cg):
        for dy, dx in PLANE:
            remote(
                part.at[cg, plane_index(dy, dx)],
                gathered.at[cg, me],
                rs_send.at[cg],
                rs_recv.at[cg],
                plane(dy, dx),
            )

    def gather(cg):
        total = part[cg, me].astype(F32)
        arrived(gathered.at[cg, 0:15], rs_recv.at[cg])
        for dy, dx in PLANE:
            total = total + gathered[cg, plane_index(dy, dx)].astype(F32)
        own[cg] = total.astype(BF16)
        for dy, dx in PLANE:
            remote(own.at[cg], factors.at[cg, me], ag_send.at[cg], ag_recv.at[cg], plane(dy, dx))
        factors[cg, me] = total.astype(BF16)

    low_half = iota((256, 128), 1) < 64
    pairs = iota((128, 256), 1) // 16 * 2

    def picked(shift, odd):
        return (iota((128, 256), 0) == pairs + (shift + odd)).astype(F32).astype(BF16)

    def spread(values, odd):
        high, low = split(values)
        return nn(high, picked(64, odd)) + nn(low, picked(64, odd))

    def against(values, w):
        high, low = split(values)
        return nt(high, w) + nt(low, w)

    def local_terms(cg):
        a_in, b_out = acc0[cg, :, 384:512], acc2[cg, :, 384:512]
        out_turned = pltpu.roll(b_out, 64, 1)
        terms[cg, 0] = spread(a_in, 0)
        terms[cg, 1] = spread(a_in, 1)
        terms[cg, 2] = against(jnp.where(low_half, out_turned, 0.0), wq0[...])
        terms[cg, 3] = against(jnp.where(low_half, 0.0, b_out), wq0[...])

    def scores(cg):
        arrived(factors.at[cg, 0:15], ag_recv.at[cg])
        b_both = factors[cg, :, 0:16].reshape(256, 128).astype(F32)
        b_turned = pltpu.roll(b_both, 64, 1)
        a_hidden = factors[cg, :, 16:24].astype(F32).reshape(128, 128).astype(BF16)

        def hidden_spread(odd):
            return jnp.concatenate([nn(a_hidden, picked(0, odd)), nn(a_hidden, picked(32, odd))], axis=0)

        even = jnp.concatenate([jnp.where(low_half, b_both, 0.0), jnp.where(low_half, b_turned, 0.0)], axis=1)
        odd = jnp.concatenate([jnp.where(low_half, 0.0, b_turned), jnp.where(low_half, 0.0, b_both)], axis=1)
        z_sum = terms[cg, 0] * nt(even.astype(BF16), wq12[...])
        z_sum += terms[cg, 1] * nt(odd.astype(BF16), wq12[...])
        z_sum += hidden_spread(0) * terms[cg, 2]
        z_sum += hidden_spread(1) * terms[cg, 3]
        high, low = split(z_sum)
        fold = (lax.rem(iota((16, 256), 1), 16) == iota((16, 256), 0)).astype(F32).astype(BF16)
        score = nt(fold, high) + nt(fold, low)
        for t in range(2):
            score_send[cg, t] = score[:, t * 128 : (t + 1) * 128]
        for pos in range(cg * 4, cg * 4 + 4):
            tile = score_send.at[cg, (pos % 4) // 2]
            for core in range(2):
                if pos != LOCAL:
                    remote(
                        tile,
                        score_recv.at[2 * pos + c],
                        sc_send,
                        sc_recv,
                        back_column(pos, core),
                    )
            if pos == LOCAL:
                remote(
                    tile,
                    score_recv.at[2 * pos + c],
                    sc_send,
                    sc_recv,
                    device(y, z * 2 + other, x),
                )
                score_recv[2 * pos + c] = score_send[cg, (pos % 4) // 2]
        share = jnp.zeros((16, 128), F32)
        for t in range(2):
            w_tile = jnp.zeros((1, 128), F32)
            for k in range(4):
                w_tile = w_tile + wrecv[cg * 8 + t * 4 + k]
            share = share + score[:, t * 128 : (t + 1) * 128] * w_tile
        return jnp.sum(share, axis=1, keepdims=True)

    def constants():
        wg[480:512] = jnp.zeros((32, 4096), BF16)
        loads["q"].wait()
        for i in range(16):
            wq0[i * 16 : (i + 1) * 16, :] = qs[:, i * 128 : (i + 1) * 128]
            wq12[i * 16 : (i + 1) * 16, 0:128] = qs[:, 2048 + i * 128 : 2048 + (i + 1) * 128]
            wq12[i * 16 : (i + 1) * 16, 128:256] = qs[:, 4096 + i * 128 : 4096 + (i + 1) * 128]
        loads["pa"].wait()
        loads["pb"].wait()
        at = iota((128, 64), 0) - iota((128, 64), 1)
        pbt1[...] = nn((at == 0).astype(F32).astype(BF16), pb[...]).astype(BF16)
        pbt2[...] = nn((at == 64).astype(F32).astype(BF16), pb[...]).astype(BF16)
        at = iota((128, 32), 0) - iota((128, 32), 1)
        pat0[...] = nn((at == 0).astype(F32).astype(BF16), pa[...]).astype(BF16)
        pat1[...] = nn((at == 32).astype(F32).astype(BF16), pa[...]).astype(BF16)

    def send_weights():
        for pos in range(NZ):
            if pos == LOCAL:
                remote(
                    wrow.at[2 * pos + other],
                    wrecv.at[2 * pos + c],
                    w_send,
                    w_recv,
                    device(y, z * 2 + other, x),
                )
                wrecv[2 * pos + c] = wrow[2 * pos + c]
            else:
                for core in range(2):
                    remote(
                        wrow.at[2 * pos + core],
                        wrecv.at[2 * pos + c],
                        w_send,
                        w_recv,
                        column(pos, core),
                    )

    chip_rows()
    slot_weights()
    constants()
    pl.semaphore_wait(passed, 4)
    send_far(2, 3)
    step_a(0)
    send_far(4)
    send_pair()
    send_near()
    send_weights()
    step_b(0)
    step_a(1)
    step_c(0)
    step_d(0, 0)
    step_a(2)
    step_b(1)
    step_d(0, 1, 2)
    step_b(2)
    step_c(1)
    step_d(0, 3)
    for name in ("pin", "pout", "wg", "wu", "wd"):
        loads[name].wait()
    chunks(0, 0, True)
    step_d(1, 0)
    step_d(1, 1, 2)
    step_c(2)
    step_d(2, 0)
    step_d(2, 1, 2)
    step_d(1, 3)
    chunks(0, 1, False)
    chunks(0, 3, False)
    arrived(full.at[:, :, 2 * NEAR : 2 * NEAR + 4], near_recv)
    arrived(full.at[:, :, 2 * LOCAL + other], pair_recv)
    chunks(1, 0, True)
    step_d(2, 3)
    chunks(1, 1, False)
    chunks(1, 3, False)
    step_e(0)
    step_e(1)
    chunks(0, 2, False)
    activations(0)
    scatter(0)
    step_e(2)
    chunks(1, 2, False)
    activations(1)
    scatter(1)
    arrived(wrecv.at[0:15], w_recv)
    local_terms(0)
    gather(0)
    local_terms(1)
    gather(1)
    total0 = scores(0)
    total = total0 + scores(1)

    on_diagonal = iota((16, 128), 0) == iota((16, 128), 1)
    row = jnp.sum(jnp.where(on_diagonal, total, 0.0), axis=0, keepdims=True)
    tot_send[...] = row
    tot_recv[2 * LOCAL + c] = row
    for pos in FAR_FIRST:
        for core in range(2):
            if pos != LOCAL:
                remote(tot_send, tot_recv.at[2 * pos + c], t_send, t_recv, back_column(pos, core))
    remote(
        tot_send,
        tot_recv.at[2 * LOCAL + c],
        t_send,
        t_recv,
        device(y, z * 2 + other, x),
    )

    arrived(score_recv.at[0:15], sc_recv)
    every = jnp.concatenate([score_recv[k] for k in range(16)], axis=1)
    high, low = split(every)
    tok_ref[...] = nn(high, wm_hi[...]) + nn(high, wm_lo[...]) + nn(low, wm_hi[...])
    arrived(tot_recv.at[0:15], t_recv)
    row = tot_recv[0]
    for k in range(1, 16):
        row = row + tot_recv[k]
    tot_ref[...] = row[:, :16]
    left(full.at[:, 0:9, 0:10], z_send)
    left(full.at[:, 0:15, 0:10], g_send)
    left(wrecv.at[0:15], w_send)
    for cg in range(2):
        left(part.at[cg, 0:15], rs_send.at[cg])
        left(factors.at[cg, 0:15], ag_send.at[cg])
    left(score_recv.at[0:15], sc_send)
    left(tot_recv.at[0:15], t_send)


def results(scores_ref, totals_ref, scores_out, totals_out):
    scores_out[...] = scores_ref[...]
    totals_out[...] = totals_ref[...] * (1.0 / math.sqrt(2048.0))


def body(inputs, cotangents, routes, gates, w_gate, w_up, w_down, proj_in, proj_out, proj_hid_a, proj_hid_b, queries):
    anywhere = pl.BlockSpec(memory_space=pl.ANY)
    vmem = pl.BlockSpec(memory_space=pltpu.VMEM)
    scores, totals = pl.pallas_call(
        kernel,
        out_shape=(jax.ShapeDtypeStruct((16, 128), F32), jax.ShapeDtypeStruct((1, 16), F32)),
        in_specs=[anywhere] * 12,
        out_specs=(vmem, vmem),
        scratch_shapes=[
            pltpu.VMEM((128, 4096), BF16),
            pltpu.VMEM((128, 4096), BF16),
            pltpu.VMEM((2, 128), I32),
            pltpu.VMEM((2, 128), F32),
            pltpu.VMEM((512, 4096), BF16),
            pltpu.VMEM((448, 4096), BF16),
            pltpu.VMEM((512, 4096), BF16),
            pltpu.VMEM((32, 448), BF16),
            pltpu.VMEM((64, 448), BF16),
            pltpu.VMEM((16, 6144), BF16),
            pltpu.VMEM((2, SHARES, 16, SLOTS, COLS), BF16),
            pltpu.VMEM((2, 10, SLOTS, COLS), BF16),
            pltpu.VMEM((2, SHARES, SLOTS, COLS), BF16),
            pltpu.VMEM((2, 4, SHARES, SLOTS, COLS), BF16),
            pltpu.VMEM((2, 256, 512), F32),
            pltpu.VMEM((2, 256, 448), F32),
            pltpu.VMEM((2, 256, 512), F32),
            pltpu.VMEM((2, 4, 256, 256), F32),
            pltpu.VMEM((128, 448), BF16),
            pltpu.VMEM((128, 448), BF16),
            pltpu.VMEM((128, 448), BF16),
            pltpu.VMEM((128, 448), BF16),
            pltpu.VMEM((256, 128), BF16),
            pltpu.VMEM((256, 256), BF16),
            pltpu.VMEM((2048, 128), BF16),
            pltpu.VMEM((2048, 128), BF16),
            pltpu.VMEM((16, 1, 128), F32),
            pltpu.VMEM((16, 1, 128), F32),
            pltpu.VMEM((2, 16, 24, 128), BF16),
            pltpu.VMEM((2, 16, 24, 128), BF16),
            pltpu.VMEM((2, 24, 128), BF16),
            pltpu.VMEM((2, 16, 24, 128), BF16),
            pltpu.VMEM((2, 2, 16, 128), F32),
            pltpu.VMEM((16, 16, 128), F32),
            pltpu.VMEM((1, 128), F32),
            pltpu.VMEM((16, 1, 128), F32),
            pltpu.SemaphoreType.DMA((12,)),
            pltpu.SemaphoreType.DMA,
            pltpu.SemaphoreType.DMA((3, 2)),
            pltpu.SemaphoreType.DMA,
            pltpu.SemaphoreType.DMA,
            pltpu.SemaphoreType.DMA,
            pltpu.SemaphoreType.DMA,
            pltpu.SemaphoreType.DMA,
            pltpu.SemaphoreType.DMA((3, 2, 13)),
            pltpu.SemaphoreType.DMA((3,)),
            pltpu.SemaphoreType.DMA((2,)),
            pltpu.SemaphoreType.DMA((2,)),
            pltpu.SemaphoreType.DMA((2,)),
            pltpu.SemaphoreType.DMA((2,)),
            pltpu.SemaphoreType.DMA,
            pltpu.SemaphoreType.DMA,
            pltpu.SemaphoreType.DMA,
            pltpu.SemaphoreType.DMA,
            pltpu.SemaphoreType.REGULAR,
        ],
        compiler_params=pltpu.CompilerParams(
            collective_id=0, has_side_effects=True, vmem_limit_bytes=60 * 1024 * 1024
        ),
    )(
        inputs,
        cotangents,
        routes.T,
        gates.T,
        w_gate[0].T,
        w_up[0].T,
        w_down[0],
        proj_in.T,
        proj_out.T,
        proj_hid_a.T,
        proj_hid_b.T,
        queries,
    )
    scores, totals = pl.pallas_call(
        results,
        out_shape=(jax.ShapeDtypeStruct((16, 128), F32), jax.ShapeDtypeStruct((1, 16), F32)),
    )(scores, totals)
    return scores.T, totals.reshape(16)


def solution(mesh):
    placed = (
        P("expert", None),
        P("expert", None),
        P("expert", None),
        P("expert", None),
        P("expert", None, ("dp", "pipe")),
        P("expert", None, ("dp", "pipe")),
        P("expert", ("dp", "pipe"), None),
        P(),
        P(),
        P(("dp", "pipe"), None),
        P(("dp", "pipe"), None),
        P(("dp", "pipe"), None),
    )
    return jax.shard_map(
        body,
        mesh=mesh,
        in_specs=placed,
        out_specs=(P("expert", ("dp", "pipe")), P(("dp", "pipe"))),
        check_vma=False,
    )
```

```python
import math

import jax
import jax.numpy as jnp
from jax import lax
from jax.experimental import pallas as pl
from jax.experimental.pallas import tpu as pltpu
from jax.sharding import PartitionSpec as P

MESH = pl.DeviceIdType.MESH
F32, BF16, I32 = jnp.float32, jnp.bfloat16, jnp.int32

NZ = 8
ORDER = (2, 6, 3, 5, 4, 0, 1, 7)
LOCAL = ORDER.index(0)
FIRST = (0, 1, LOCAL, 6, 7)
NEAR = 6
SLOTS = 32
COLS = 256
SHARES = 16
GROUPS = ((0, 4), (4, 4), (8, 2))
PIECES = (0, -1, 1, 2)
PLANE = sorted(
    ((dy, dx) for dy in range(4) for dx in range(4) if dy or dx),
    key=lambda o: -min(o[0], 4 - o[0]) - min(o[1], 4 - o[1]),
)
FAR_FIRST = sorted(range(NZ), key=lambda i: -min(ORDER[i], NZ - ORDER[i]))


def nn(a, b):
    return lax.dot_general(a, b, (((1,), (0,)), ((), ())), preferred_element_type=F32)


def nt(a, b):
    return lax.dot_general(a, b, (((1,), (1,)), ((), ())), preferred_element_type=F32)


def iota(shape, dim):
    return lax.broadcasted_iota(I32, shape, dim)


def split(v):
    high = v.astype(BF16)
    return high, (v - high.astype(F32)).astype(BF16)


def kernel(
    x_hbm, g_hbm, routes_hbm, gates_hbm, wg_hbm, wu_hbm, wd_hbm, pin_hbm, pout_hbm, pa_hbm, pb_hbm, q_hbm,
    tok_ref, tot_ref,
    xs, gs, routes, gates, wg, wu, wd, pa, pb, qs,
    full, out_rows, out_pair, out_near, acc0, acc1, acc2, terms,
    pat0, pat1, pbt1, pbt2, wq0, wq12, wm_hi, wm_lo, wrow, wrecv,
    part, gathered, own, factors, score_send, score_recv, tot_send, tot_recv,
    load_sem, z_send, z_recv, pair_recv, near_recv, w_send, w_recv,
    g_send, g_recv, e_recv, rs_send, rs_recv, ag_send, ag_recv, sc_send, sc_recv, t_send, t_recv,
    passed,
):
    y, e, x = lax.axis_index("dp"), lax.axis_index("expert"), lax.axis_index("pipe")
    z, c = lax.div(e, 2), lax.rem(e, 2)
    other = 1 - c
    me = y * 4 + x

    def device(yy, ee, xx):
        return {"dp": yy, "expert": ee, "pipe": xx}

    def column(pos, core):
        return device(y, lax.rem(z + ORDER[pos], NZ) * 2 + core, x)

    def back_column(pos, core):
        return device(y, lax.rem(z + NZ - ORDER[pos], NZ) * 2 + core, x)

    def plane(dy, dx):
        return device(lax.rem(y + dy, 4), e, lax.rem(x + dx, 4))

    def plane_index(dy, dx):
        return lax.rem(y + dy, 4) * 4 + lax.rem(x + dx, 4)

    def remote(src, dst, ss, rs, dev):
        pltpu.make_async_remote_copy(
            src_ref=src, dst_ref=dst, send_sem=ss, recv_sem=rs, device_id=dev, device_id_type=MESH
        ).start()

    def arrived(dst, rs):
        pltpu.make_async_remote_copy(
            src_ref=dst, dst_ref=dst, send_sem=rs, recv_sem=rs, device_id=device(y, e, x), device_id_type=MESH
        ).wait_recv()

    def left(src, ss):
        pltpu.make_async_remote_copy(
            src_ref=src, dst_ref=src, send_sem=ss, recv_sem=ss, device_id=device(y, e, x), device_id_type=MESH
        ).wait_send()

    barrier = pltpu.get_barrier_semaphore()
    for dy, dx in ((0, 1), (0, 3), (1, 0), (3, 0)):
        pl.semaphore_signal(barrier, inc=1, device_id=plane(dy, dx), device_id_type=MESH)
    for pos in FIRST:
        if pos == LOCAL:
            pl.semaphore_signal(barrier, inc=1, device_id=column(pos, other), device_id_type=MESH)
        else:
            for core in range(2):
                pl.semaphore_signal(barrier, inc=1, device_id=column(pos, core), device_id_type=MESH)

    loads = {}
    for i, (name, src, dst) in enumerate(
        (
            ("routes", routes_hbm, routes),
            ("gates", gates_hbm, gates),
            ("x", x_hbm, xs),
            ("g", g_hbm, gs),
            ("q", q_hbm, qs),
            ("pa", pa_hbm, pa),
            ("pb", pb_hbm, pb),
            ("pin", pin_hbm, wg.at[448:480]),
            ("pout", pout_hbm, wd.at[448:512]),
            ("wg", wg_hbm, wg.at[0:448]),
            ("wu", wu_hbm, wu),
            ("wd", wd_hbm, wd.at[0:448]),
        )
    ):
        loads[name] = pltpu.make_async_copy(src, dst, load_sem.at[i])
        loads[name].start()

    loads["routes"].wait()
    loads["gates"].wait()
    first, second = routes[0:1, :], routes[1:2, :]
    expert_rows = iota((16, 128), 0)
    named = ((expert_rows == first) | (expert_rows == second)).astype(F32)
    before = (iota((128, 128), 0) < iota((128, 128), 1)).astype(F32)
    earlier = nn(named.astype(BF16), before.astype(BF16))

    def places(route):
        slot = jnp.sum(jnp.where(expert_rows == route, earlier, 0.0), axis=0, keepdims=True).astype(I32)
        offset = ((route >> 1) - z) & (NZ - 1)
        pos = jnp.zeros_like(offset)
        for i, o in enumerate(ORDER):
            pos = jnp.where(offset == o, i, pos)
        block = pos * 2 + (route & 1)
        lane = block * 128 + ((pos & 1) * 2 + c) * 32 + slot
        return block * SLOTS + slot, lane

    place0, lane0 = places(first)
    place1, lane1 = places(second)

    def picks_of(start, count):
        rows = iota((count, 128), 0) + start
        return ((rows == place0) | (rows == place1)).astype(F32).astype(BF16)

    far = 10 * SLOTS
    picks = picks_of(0, far)
    shares = (y * 4 + x, x * 4 + y)
    for a, (name, source) in enumerate((("x", xs), ("g", gs))):
        loads[name].wait()
        columns = pl.ds(pl.multiple_of(shares[a] * COLS, COLS), COLS)
        rows = nn(picks, source[:, columns]).astype(BF16)
        out_rows[a] = rows.reshape(10, SLOTS, COLS)

    pl.semaphore_wait(barrier, 13)

    def send_far(*positions):
        for pos in positions:
            for a in range(2):
                for core in range(2):
                    remote(
                        out_rows.at[a, 2 * pos + core],
                        full.at[a, shares[a], 2 * pos + c],
                        z_send,
                        z_recv.at[pos // 2, a],
                        column(pos, core),
                    )

    send_far(0, 1)
    for pos in range(NEAR, NZ):
        for core in range(2):
            pl.semaphore_signal(passed, inc=1, device_id=column(pos, core), device_id_type=MESH)

    near_picks = picks_of(2 * NEAR * SLOTS, 4 * SLOTS)
    for a, source in enumerate((xs, gs)):
        for p in range(SHARES):
            rows = nn(near_picks, source[:, p * COLS : (p + 1) * COLS]).astype(BF16)
            out_near[a, :, p] = rows.reshape(4, SLOTS, COLS)

    def send_near():
        for a in range(2):
            for core in range(2):
                for pos in range(NEAR, NZ):
                    k = 2 * (pos - NEAR)
                    remote(
                        out_near.at[a, k + core],
                        full.at[a, :, 2 * pos + c],
                        z_send,
                        near_recv,
                        column(pos, core),
                    )

    def chip_rows():
        pair_picks = picks_of((2 * LOCAL + other) * SLOTS, SLOTS)
        own_picks = picks_of((2 * LOCAL + c) * SLOTS, SLOTS)
        for a, source in enumerate((xs, gs)):
            for p in range(SHARES):
                columns = source[:, p * COLS : (p + 1) * COLS]
                out_pair[a, p] = nn(pair_picks, columns).astype(BF16)
                full[a, p, 2 * LOCAL + c] = nn(own_picks, columns).astype(BF16)

    def send_pair():
        for a in range(2):
            remote(
                out_pair.at[a],
                full.at[a, :, 2 * LOCAL + c],
                z_send,
                pair_recv,
                device(y, z * 2 + other, x),
            )

    def slot_weights():
        lanes = iota((2048, 128), 0)
        weights = jnp.where(lanes == lane0, gates[0:1, :], 0.0) + jnp.where(lanes == lane1, gates[1:2, :], 0.0)
        high, low = split(weights)
        wm_hi[...] = high
        wm_lo[...] = low
        ones = jnp.ones((8, 128), BF16)
        sums = nt(ones, high) + nt(ones, low)
        for k in range(16):
            wrow[k] = sums[0:1, k * 128 : (k + 1) * 128]

    def ring(a, major, minor):
        major, minor = lax.rem(major + 4, 4), lax.rem(minor + 4, 4)
        return device(major, e, minor) if a == 0 else device(minor, e, major)

    mine = ((y, x), (x, y))

    def share_ref(a, dmajor, dminor, first_block, blocks):
        major, minor = mine[a]
        share = lax.rem(major + dmajor + 4, 4) * 4 + lax.rem(minor + dminor + 4, 4)
        return full.at[a, share, pl.ds(first_block, blocks)]

    def send_group(a, ref, sem, dmajor, dminor):
        major, minor = mine[a]
        remote(ref, ref, g_send, sem, ring(a, major + dmajor, minor + dminor))

    def send_piece(g, a, piece):
        b, n = GROUPS[g]
        for way, d in enumerate((1, -1)):
            send_group(a, share_ref(a, 0, PIECES[piece], b, n), g_recv.at[g, a, 3 + 2 * piece + way], d, 0)

    def step_a(g):
        b, n = GROUPS[g]
        h = n // 2
        for a in range(2):
            arrived(share_ref(a, 0, 0, b, n), z_recv.at[g, a])
            for tag, first in ((0, b), (1, b + h)):
                other_half = b + h if tag == 0 else b
                d = 1 if tag == 0 else -1
                send_group(a, share_ref(a, 0, 0, first, h), g_recv.at[g, a, tag], 0, d)
                send_group(a, share_ref(a, 0, 0, other_half, h), g_recv.at[g, a, 11 + tag], 0, d)
        if g == 0:
            for a in range(2):
                send_piece(g, a, 0)

    def step_b(g):
        b, n = GROUPS[g]
        h = n // 2
        for a in range(2):
            arrived(share_ref(a, 0, -1, b, h), g_recv.at[g, a, 0])
            send_group(a, share_ref(a, 0, -1, b, h), g_recv.at[g, a, 2], 0, 1)
            arrived(share_ref(a, 0, 1, b + h, h), g_recv.at[g, a, 1])
            send_group(a, share_ref(a, 0, 1, b + h, h), g_recv.at[g, a, 2], 0, -1)
        for a in range(2):
            arrived(share_ref(a, 0, -1, b + h, h), g_recv.at[g, a, 11])
            arrived(share_ref(a, 0, 1, b, h), g_recv.at[g, a, 12])
            for piece in (1, 2) if g == 0 else (0, 1, 2):
                send_piece(g, a, piece)

    def step_c(g):
        b, n = GROUPS[g]
        for a in range(2):
            arrived(share_ref(a, 0, 2, b, n), g_recv.at[g, a, 2])
            send_piece(g, a, 3)

    def step_d(g, *pieces):
        b, n = GROUPS[g]
        h = n // 2
        for piece in pieces:
            dm, tag = PIECES[piece], 3 + 2 * piece
            for a in range(2):
                arrived(share_ref(a, -1, dm, b, n), g_recv.at[g, a, tag])
                send_group(a, share_ref(a, -1, dm, b, h), e_recv.at[g], 1, 0)
                arrived(share_ref(a, 1, dm, b, n), g_recv.at[g, a, tag + 1])
                send_group(a, share_ref(a, 1, dm, b + h, h), e_recv.at[g], -1, 0)

    def step_e(g):
        b, n = GROUPS[g]
        arrived(full.at[:, 0:4, pl.ds(b, n)], e_recv.at[g])

    def rows_of(a, chunk, b0):
        return jnp.concatenate([full[a, chunk * 4 + i, b0 : b0 + 8].reshape(256, COLS) for i in range(4)], axis=1)

    def chunk_in(cg, chunk, begin):
        ks = pl.ds(pl.multiple_of(chunk * 1024, 1024), 1024)
        rows = rows_of(0, chunk, cg * 8)
        for acc, w in ((acc0, wg), (acc1, wu)):
            v = nt(rows, w[:, ks])
            acc[cg] = v if begin else acc[cg] + v

    def chunk_back(cg, chunk, begin):
        ks = pl.ds(pl.multiple_of(chunk * 1024, 1024), 1024)
        v = nt(rows_of(1, chunk, cg * 8), wd[:, ks])
        acc2[cg] = v if begin else acc2[cg] + v

    def chunks(cg, offset, begin):
        chunk_in(cg, lax.rem(y + offset, 4), begin)
        chunk_back(cg, lax.rem(x + offset, 4), begin)

    def activations(cg):
        gate, up, back = acc0[cg, :, :448], acc1[cg], acc2[cg, :, :448]
        s = jax.nn.sigmoid(gate)
        gated = gate * s
        hidden = (gated * up).astype(BF16)
        d_up = (back * gated).astype(BF16)
        d_gate = (back * up * s * (1.0 + gate * (1.0 - s))).astype(BF16)
        grads = nt(d_up, pbt1[...]) + nt(d_gate, pbt2[...])
        halves = nt(hidden[0:128], pat0[...]) + nt(hidden[128:256], pat1[...])
        part[cg, :, 0:16] = grads.reshape(16, 16, 128).astype(BF16)
        part[cg, :, 16:24] = halves.reshape(16, 8, 128).astype(BF16)

    def scatter(cg):
        for dy, dx in PLANE:
            remote(
                part.at[cg, plane_index(dy, dx)],
                gathered.at[cg, me],
                rs_send.at[cg],
                rs_recv.at[cg],
                plane(dy, dx),
            )

    def gather(cg):
        total = part[cg, me].astype(F32)
        arrived(gathered.at[cg, 0:15], rs_recv.at[cg])
        for dy, dx in PLANE:
            total = total + gathered[cg, plane_index(dy, dx)].astype(F32)
        own[cg] = total.astype(BF16)
        for dy, dx in PLANE:
            remote(own.at[cg], factors.at[cg, me], ag_send.at[cg], ag_recv.at[cg], plane(dy, dx))
        factors[cg, me] = total.astype(BF16)

    low_half = iota((256, 128), 1) < 64
    pairs = iota((128, 256), 1) // 16 * 2

    def picked(shift, odd):
        return (iota((128, 256), 0) == pairs + (shift + odd)).astype(F32).astype(BF16)

    def spread(values, odd):
        high, low = split(values)
        return nn(high, picked(64, odd)) + nn(low, picked(64, odd))

    def against(values, w):
        high, low = split(values)
        return nt(high, w) + nt(low, w)

    def local_terms(cg):
        a_in, b_out = acc0[cg, :, 384:512], acc2[cg, :, 384:512]
        out_turned = pltpu.roll(b_out, 64, 1)
        terms[cg, 0] = spread(a_in, 0)
        terms[cg, 1] = spread(a_in, 1)
        terms[cg, 2] = against(jnp.where(low_half, out_turned, 0.0), wq0[...])
        terms[cg, 3] = against(jnp.where(low_half, 0.0, b_out), wq0[...])

    def scores(cg):
        arrived(factors.at[cg, 0:15], ag_recv.at[cg])
        b_both = factors[cg, :, 0:16].reshape(256, 128).astype(F32)
        b_turned = pltpu.roll(b_both, 64, 1)
        a_hidden = factors[cg, :, 16:24].astype(F32).reshape(128, 128).astype(BF16)

        def hidden_spread(odd):
            return jnp.concatenate([nn(a_hidden, picked(0, odd)), nn(a_hidden, picked(32, odd))], axis=0)

        even = jnp.concatenate([jnp.where(low_half, b_both, 0.0), jnp.where(low_half, b_turned, 0.0)], axis=1)
        odd = jnp.concatenate([jnp.where(low_half, 0.0, b_turned), jnp.where(low_half, 0.0, b_both)], axis=1)
        z_sum = terms[cg, 0] * nt(even.astype(BF16), wq12[...])
        z_sum += terms[cg, 1] * nt(odd.astype(BF16), wq12[...])
        z_sum += hidden_spread(0) * terms[cg, 2]
        z_sum += hidden_spread(1) * terms[cg, 3]
        high, low = split(z_sum)
        fold = (lax.rem(iota((16, 256), 1), 16) == iota((16, 256), 0)).astype(F32).astype(BF16)
        score = nt(fold, high) + nt(fold, low)
        for t in range(2):
            score_send[cg, t] = score[:, t * 128 : (t + 1) * 128]
        for pos in range(cg * 4, cg * 4 + 4):
            tile = score_send.at[cg, (pos % 4) // 2]
            for core in range(2):
                if pos != LOCAL:
                    remote(
                        tile,
                        score_recv.at[2 * pos + c],
                        sc_send,
                        sc_recv.at[cg],
                        back_column(pos, core),
                    )
            if pos == LOCAL:
                remote(
                    tile,
                    score_recv.at[2 * pos + c],
                    sc_send,
                    sc_recv.at[cg],
                    device(y, z * 2 + other, x),
                )
                score_recv[2 * pos + c] = score_send[cg, (pos % 4) // 2]
        share = jnp.zeros((16, 128), F32)
        for t in range(2):
            w_tile = jnp.zeros((1, 128), F32)
            for k in range(4):
                w_tile = w_tile + wrecv[cg * 8 + t * 4 + k]
            share = share + score[:, t * 128 : (t + 1) * 128] * w_tile
        return jnp.sum(share, axis=1, keepdims=True)

    def constants():
        wg[480:512] = jnp.zeros((32, 4096), BF16)
        loads["q"].wait()
        for i in range(16):
            wq0[i * 16 : (i + 1) * 16, :] = qs[:, i * 128 : (i + 1) * 128]
            wq12[i * 16 : (i + 1) * 16, 0:128] = qs[:, 2048 + i * 128 : 2048 + (i + 1) * 128]
            wq12[i * 16 : (i + 1) * 16, 128:256] = qs[:, 4096 + i * 128 : 4096 + (i + 1) * 128]
        loads["pa"].wait()
        loads["pb"].wait()
        at = iota((128, 64), 0) - iota((128, 64), 1)
        pbt1[...] = nn((at == 0).astype(F32).astype(BF16), pb[...]).astype(BF16)
        pbt2[...] = nn((at == 64).astype(F32).astype(BF16), pb[...]).astype(BF16)
        at = iota((128, 32), 0) - iota((128, 32), 1)
        pat0[...] = nn((at == 0).astype(F32).astype(BF16), pa[...]).astype(BF16)
        pat1[...] = nn((at == 32).astype(F32).astype(BF16), pa[...]).astype(BF16)

    def send_weights():
        for pos in range(NZ):
            if pos == LOCAL:
                remote(
                    wrow.at[2 * pos + other],
                    wrecv.at[2 * pos + c],
                    w_send,
                    w_recv,
                    device(y, z * 2 + other, x),
                )
                wrecv[2 * pos + c] = wrow[2 * pos + c]
            else:
                for core in range(2):
                    remote(
                        wrow.at[2 * pos + core],
                        wrecv.at[2 * pos + c],
                        w_send,
                        w_recv,
                        column(pos, core),
                    )

    chip_rows()
    slot_weights()
    constants()
    pl.semaphore_wait(passed, 4)
    send_far(2, 3)
    step_a(0)
    send_far(4)
    send_pair()
    send_near()
    send_weights()
    step_b(0)
    step_a(1)
    step_c(0)
    step_d(0, 0)
    step_a(2)
    step_b(1)
    step_d(0, 1, 2)
    step_b(2)
    step_c(1)
    step_d(0, 3)
    for name in ("pin", "pout", "wg", "wu", "wd"):
        loads[name].wait()
    chunks(0, 0, True)
    step_d(1, 0)
    step_d(1, 1, 2)
    step_c(2)
    step_d(2, 0)
    step_d(2, 1, 2)
    step_d(1, 3)
    chunks(0, 1, False)
    chunks(0, 3, False)
    arrived(full.at[:, :, 2 * NEAR : 2 * NEAR + 4], near_recv)
    arrived(full.at[:, :, 2 * LOCAL + other], pair_recv)
    chunks(1, 0, True)
    step_d(2, 3)
    chunks(1, 1, False)
    chunks(1, 3, False)
    step_e(0)
    step_e(1)
    chunks(0, 2, False)
    activations(0)
    scatter(0)
    step_e(2)
    chunks(1, 2, False)
    activations(1)
    scatter(1)
    arrived(wrecv.at[0:15], w_recv)
    local_terms(0)
    gather(0)
    local_terms(1)
    gather(1)
    total0 = scores(0)
    total = total0 + scores(1)

    on_diagonal = iota((16, 128), 0) == iota((16, 128), 1)
    row = jnp.sum(jnp.where(on_diagonal, total, 0.0), axis=0, keepdims=True)
    tot_send[...] = row
    tot_recv[2 * LOCAL + c] = row
    for pos in FAR_FIRST:
        for core in range(2):
            if pos != LOCAL:
                remote(tot_send, tot_recv.at[2 * pos + c], t_send, t_recv, back_column(pos, core))
    remote(
        tot_send,
        tot_recv.at[2 * LOCAL + c],
        t_send,
        t_recv,
        device(y, z * 2 + other, x),
    )

    def combined(first):
        every = jnp.concatenate([score_recv[k] for k in range(first, first + 8)], axis=1)
        high, low = split(every)
        slots = pl.ds(first * 128, 1024)
        return nn(high, wm_hi[slots]) + nn(high, wm_lo[slots]) + nn(low, wm_hi[slots])

    arrived(score_recv.at[0:8], sc_recv.at[0])
    tok_ref[...] = combined(0)
    arrived(score_recv.at[8:15], sc_recv.at[1])
    tok_ref[...] = tok_ref[...] + combined(8)
    arrived(tot_recv.at[0:15], t_recv)
    row = tot_recv[0]
    for k in range(1, 16):
        row = row + tot_recv[k]
    tot_ref[...] = row[:, :16]
    left(full.at[:, 0:9, 0:10], z_send)
    left(full.at[:, 0:15, 0:10], g_send)
    left(wrecv.at[0:15], w_send)
    for cg in range(2):
        left(part.at[cg, 0:15], rs_send.at[cg])
        left(factors.at[cg, 0:15], ag_send.at[cg])
    left(score_recv.at[0:15], sc_send)
    left(tot_recv.at[0:15], t_send)


def results(scores_ref, totals_ref, scores_out, totals_out):
    scores_out[...] = scores_ref[...]
    totals_out[...] = totals_ref[...] * (1.0 / math.sqrt(2048.0))


def body(inputs, cotangents, routes, gates, w_gate, w_up, w_down, proj_in, proj_out, proj_hid_a, proj_hid_b, queries):
    anywhere = pl.BlockSpec(memory_space=pl.ANY)
    vmem = pl.BlockSpec(memory_space=pltpu.VMEM)
    scores, totals = pl.pallas_call(
        kernel,
        out_shape=(jax.ShapeDtypeStruct((16, 128), F32), jax.ShapeDtypeStruct((1, 16), F32)),
        in_specs=[anywhere] * 12,
        out_specs=(vmem, vmem),
        scratch_shapes=[
            pltpu.VMEM((128, 4096), BF16),
            pltpu.VMEM((128, 4096), BF16),
            pltpu.VMEM((2, 128), I32),
            pltpu.VMEM((2, 128), F32),
            pltpu.VMEM((512, 4096), BF16),
            pltpu.VMEM((448, 4096), BF16),
            pltpu.VMEM((512, 4096), BF16),
            pltpu.VMEM((32, 448), BF16),
            pltpu.VMEM((64, 448), BF16),
            pltpu.VMEM((16, 6144), BF16),
            pltpu.VMEM((2, SHARES, 16, SLOTS, COLS), BF16),
            pltpu.VMEM((2, 10, SLOTS, COLS), BF16),
            pltpu.VMEM((2, SHARES, SLOTS, COLS), BF16),
            pltpu.VMEM((2, 4, SHARES, SLOTS, COLS), BF16),
            pltpu.VMEM((2, 256, 512), F32),
            pltpu.VMEM((2, 256, 448), F32),
            pltpu.VMEM((2, 256, 512), F32),
            pltpu.VMEM((2, 4, 256, 256), F32),
            pltpu.VMEM((128, 448), BF16),
            pltpu.VMEM((128, 448), BF16),
            pltpu.VMEM((128, 448), BF16),
            pltpu.VMEM((128, 448), BF16),
            pltpu.VMEM((256, 128), BF16),
            pltpu.VMEM((256, 256), BF16),
            pltpu.VMEM((2048, 128), BF16),
            pltpu.VMEM((2048, 128), BF16),
            pltpu.VMEM((16, 1, 128), F32),
            pltpu.VMEM((16, 1, 128), F32),
            pltpu.VMEM((2, 16, 24, 128), BF16),
            pltpu.VMEM((2, 16, 24, 128), BF16),
            pltpu.VMEM((2, 24, 128), BF16),
            pltpu.VMEM((2, 16, 24, 128), BF16),
            pltpu.VMEM((2, 2, 16, 128), F32),
            pltpu.VMEM((16, 16, 128), F32),
            pltpu.VMEM((1, 128), F32),
            pltpu.VMEM((16, 1, 128), F32),
            pltpu.SemaphoreType.DMA((12,)),
            pltpu.SemaphoreType.DMA,
            pltpu.SemaphoreType.DMA((3, 2)),
            pltpu.SemaphoreType.DMA,
            pltpu.SemaphoreType.DMA,
            pltpu.SemaphoreType.DMA,
            pltpu.SemaphoreType.DMA,
            pltpu.SemaphoreType.DMA,
            pltpu.SemaphoreType.DMA((3, 2, 13)),
            pltpu.SemaphoreType.DMA((3,)),
            pltpu.SemaphoreType.DMA((2,)),
            pltpu.SemaphoreType.DMA((2,)),
            pltpu.SemaphoreType.DMA((2,)),
            pltpu.SemaphoreType.DMA((2,)),
            pltpu.SemaphoreType.DMA,
            pltpu.SemaphoreType.DMA((2,)),
            pltpu.SemaphoreType.DMA,
            pltpu.SemaphoreType.DMA,
            pltpu.SemaphoreType.REGULAR,
        ],
        compiler_params=pltpu.CompilerParams(
            collective_id=0, has_side_effects=True, vmem_limit_bytes=60 * 1024 * 1024
        ),
    )(
        inputs,
        cotangents,
        routes.T,
        gates.T,
        w_gate[0].T,
        w_up[0].T,
        w_down[0],
        proj_in.T,
        proj_out.T,
        proj_hid_a.T,
        proj_hid_b.T,
        queries,
    )
    scores, totals = pl.pallas_call(
        results,
        out_shape=(jax.ShapeDtypeStruct((16, 128), F32), jax.ShapeDtypeStruct((1, 16), F32)),
    )(scores, totals)
    return scores.T, totals.reshape(16)


def solution(mesh):
    placed = (
        P("expert", None),
        P("expert", None),
        P("expert", None),
        P("expert", None),
        P("expert", None, ("dp", "pipe")),
        P("expert", None, ("dp", "pipe")),
        P("expert", ("dp", "pipe"), None),
        P(),
        P(),
        P(("dp", "pipe"), None),
        P(("dp", "pipe"), None),
        P(("dp", "pipe"), None),
    )
    return jax.shard_map(
        body,
        mesh=mesh,
        in_specs=placed,
        out_specs=(P("expert", ("dp", "pipe")), P(("dp", "pipe"))),
        check_vma=False,
    )
```
